32 devices in a mesh: row: 8 (over y, x, core), col: 4 (over z).
Axes of the slice: x: 2, y: 2, z: 4, core: 2. Of those that a mesh axis runs over, the one named last changes fastest.
Arguments:
- columns: float32 [4096, 8192], P('col', 'row'), may hold values from -64 to 64
- block_order: int32 [64], P('col'), may hold values from 0 to 63, as said below
Outputs:
- rotated: float32 [4096, 8192], P('col', 'row')
The draws below stay inside these ranges and needn't reach their ends.
Inputs may be any that keep to these rules, and one draw needn't show every extreme that they name: block_order is a permutation of 0 .. 63 in which slots c * 16 to (c + 1) * 16 - 1 name blocks c * 16 to (c + 1) * 16 - 1.
All inputs are finite; a program needn't handle non-finite values.
Results may differ from the reference program's by a relative error of at most 0.00055.
Values sent between devices are 32-bit elements; how exact they have to be, the bound alone decides.
A program may use at most 64 MiB of HBM per device.

```python
import math
import jax
import jax.numpy as jnp
from jax import lax

BLOCK = 64
STEPS = 4
BLOCKS_DEV = 16
N = 4096
M = 8192
BLOCKS = 64


def draw_columns(key, part):
    keys = jax.random.split(key, 4)
    gain_rows = 1.0 + 2.0 * jnp.arange(M, dtype=jnp.float32) / M
    loadings = jax.random.truncated_normal(keys[2], -3.0, 3.0, (N,), jnp.float32)
    noise = jax.random.truncated_normal(keys[0], -4.0, 4.0, (N, M), jnp.float32)
    scales = jnp.exp(jax.random.uniform(keys[1], (N,), jnp.float32, math.log(0.3), math.log(3.0)))
    common = jax.random.truncated_normal(keys[3], -3.0, 3.0, (M,), jnp.float32)
    return noise * scales[:, None] + loadings[:, None] * (common * gain_rows)[None, :]


def draw_block_order(key, part):
    groups = BLOCKS // BLOCKS_DEV
    scores = jax.random.randint(key, (groups, BLOCKS_DEV), 0, 1 << 20) * BLOCKS_DEV + jnp.arange(BLOCKS_DEV, dtype=jnp.int32)[None, :]
    shuffled = jnp.argsort(scores, axis=1, stable=True).astype(jnp.int32)
    return (shuffled + (jnp.arange(groups, dtype=jnp.int32) * BLOCKS_DEV)[:, None]).reshape(-1)


def setup_inputs(seed: int = 0) -> dict:
    splits = jax.random.split(jax.random.key(seed), 3)
    return {
        "columns": draw_columns(jax.random.fold_in(splits[2], 71), 0),
        "block_order": draw_block_order(jax.random.fold_in(splits[2], 71), 0),
    }


def cayley_turn(cross_sum, col_norms):
    highest = lax.Precision.HIGHEST
    top_norms = col_norms[:, :BLOCK][:, :, None]
    bottom_norms = col_norms[:, BLOCK:][:, None, :]
    spread = bottom_norms - top_norms
    radius = jnp.sqrt(spread * spread + 4.0 * cross_sum * cross_sum)
    scale_term = (top_norms + bottom_norms) / BLOCK
    coupling = 2.0 * cross_sum * spread / (spread * spread + 4.0 * cross_sum * cross_sum + jnp.abs(spread) * radius + scale_term * scale_term)
    identity = jnp.eye(BLOCK, dtype=jnp.float32)
    left_system = identity + jnp.einsum('pij,pkj->pik', coupling, coupling, precision=highest)
    right_system = identity + jnp.einsum('pji,pjk->pik', coupling, coupling, precision=highest)
    left_factor = jnp.linalg.cholesky(left_system)
    right_factor = jnp.linalg.cholesky(right_system)
    identities = jnp.broadcast_to(identity, coupling.shape)
    upper_half = jnp.concatenate([identities, coupling], axis=2)
    lower_half = jnp.concatenate([-jnp.transpose(coupling, (0, 2, 1)), identities], axis=2)

    def solve_one(factor, target):
        return jax.scipy.linalg.cho_solve((factor, True), target)
    upper_solved = jax.vmap(solve_one)(left_factor, upper_half)
    lower_solved = jax.vmap(solve_one)(right_factor, lower_half)
    solved = jnp.concatenate([upper_solved, lower_solved], axis=1)
    plus_skew = jnp.concatenate([upper_half, lower_half], axis=1)
    return jnp.einsum('pij,pjk->pik', plus_skew, solved, precision=highest)

def reference(columns, block_order):
    highest = lax.Precision.HIGHEST
    width, length = columns.shape
    count = width // BLOCK
    blocks = jnp.take(columns.reshape(count, BLOCK, length), block_order.astype(jnp.int32), axis=0)
    blocks = blocks.reshape(count // 2, 2 * BLOCK, length)
    for sweep_step in range(STEPS):
        gram_sum = jnp.einsum('pim,pjm->pij', blocks, blocks, precision=highest)
        col_norms = jnp.diagonal(gram_sum, axis1=1, axis2=2)
        cross_sum = gram_sum[:, :BLOCK, BLOCK:]
        turn_matrix = cayley_turn(cross_sum, col_norms)
        turned = jnp.einsum('pij,pim->pjm', turn_matrix, blocks, precision=highest)
        top_blocks = turned[:, :BLOCK]
        bottom_blocks = turned[:, BLOCK:]
        new_tops = jnp.concatenate([top_blocks[:1], bottom_blocks[:1], top_blocks[1:-1]], axis=0)
        new_bottoms = jnp.concatenate([bottom_blocks[1:], top_blocks[-1:]], axis=0)
        blocks = jnp.concatenate([new_tops, new_bottoms], axis=1)
    return blocks.reshape(width, length)
```

```python
import functools

import jax
import jax.numpy as jnp
from jax import lax
from jax.experimental import pallas as pl
from jax.experimental.pallas import tpu as pltpu
from jax.sharding import PartitionSpec as P

BLOCK = 64
PAIR = 2 * BLOCK
STEPS = 4
HALF = BLOCK // 2
PACKED = HALF + 8
UPPER = 1.0 + BLOCK * BLOCK * 0.0905
NN = (((1,), (0,)), ((), ()))
NT = (((1,), (1,)), ((), ()))


def split(a):
    high = a.astype(jnp.bfloat16)
    return high, (a - high.astype(jnp.float32)).astype(jnp.bfloat16)


def split3(a):
    high = a.astype(jnp.bfloat16)
    rest = a - high.astype(jnp.float32)
    middle = rest.astype(jnp.bfloat16)
    return high, middle, (rest - middle.astype(jnp.float32)).astype(jnp.bfloat16)


def product(a, b, dims=NN):
    return lax.dot_general(a, b, dims, preferred_element_type=jnp.float32)


def mm3(a, b):
    (ah, am), (bh, bm) = split(a), split(b)
    count = a.shape[0]
    stacked = product(jnp.concatenate([ah, am], axis=0), bh)
    return stacked[:count] + stacked[count:] + product(ah, bm)


def mm6(a, b, dims=NN):
    (ah, am, al), (bh, bm, bl) = split3(a), split3(b)
    count = a.shape[0]
    first = product(jnp.concatenate([ah, am, al], axis=0), bh, dims)
    second = product(jnp.concatenate([ah, am], axis=0), bm, dims)
    small = first[2 * count :] + second[count:] + product(ah, bl, dims)
    return first[:count] + ((first[count : 2 * count] + second[:count]) + small)


def left(a):
    return a[:, :BLOCK]


def inverse(system, eye):
    low = 2.0 / (1.0 + UPPER)
    y = system * low
    reach = low * (2.0 - low)
    scale = 2.0 / (1.0 + reach)
    x = (scale * low) * (2.0 * eye - y)
    y = scale * (2.0 * y - mm3(left(y), y))
    low = scale * reach
    while low < 0.999:
        reach = low * (2.0 - low)
        scale = 2.0 / (1.0 + reach)
        following = scale * (2.0 * y - mm3(left(y), y))
        x = scale * (2.0 * x - mm3(left(x), y))
        y = following
        low = scale * reach
    return x


def turn_packed(total):
    row = lax.broadcasted_iota(jnp.int32, (HALF, PAIR), 0)
    lane = lax.broadcasted_iota(jnp.int32, (HALF, PAIR), 1)
    cross = total[:HALF]
    norms = total[HALF : HALF + 1]
    bottom_norms = total[HALF + 1 : HALF + 2]
    upper_norms = jnp.sum(jnp.where(lane == row, norms, 0.0), axis=1, keepdims=True)
    lower_norms = jnp.sum(jnp.where(lane == row + HALF, norms, 0.0), axis=1, keepdims=True)
    top_norms = jnp.where(lane < BLOCK, upper_norms, lower_norms)
    spread = bottom_norms - top_norms
    square = spread * spread + 4.0 * cross * cross
    radius = jnp.sqrt(square)
    scale_term = (top_norms + bottom_norms) / BLOCK
    packed = 2.0 * cross * spread / (square + jnp.abs(spread) * radius + scale_term * scale_term)
    rolled = pltpu.roll(packed, BLOCK, 1)
    coupling = jnp.concatenate([jnp.where(lane < BLOCK, packed, rolled), jnp.where(lane < BLOCK, rolled, packed)], axis=0)
    rows = lax.broadcasted_iota(jnp.int32, (BLOCK, PAIR), 0)
    lanes = lax.broadcasted_iota(jnp.int32, (BLOCK, PAIR), 1)
    columns = jnp.where(lanes < BLOCK, lanes, lanes - BLOCK)
    eye = jnp.where(rows == columns, 1.0, 0.0).astype(jnp.float32)
    narrow = left(coupling)
    narrow_t = narrow.T
    system = eye + mm6(narrow, jnp.concatenate([narrow, narrow], axis=0), NT)
    x = inverse(system, eye)
    lower = mm6(narrow_t, x)
    residual = eye - x - mm6(narrow, lower)
    stacked = jnp.concatenate([x, lower], axis=0)
    stacked = stacked + mm3(left(stacked), residual)
    x, lower = stacked[:BLOCK], 2.0 * stacked[BLOCK:]
    corner = eye - mm6(left(lower), coupling)
    diagonal = jnp.sum(jnp.where(rows == columns, corner, 0.0), axis=0, keepdims=True)
    mixed = jnp.where(rows <= columns, 2.0 * x - eye, corner)
    body = jnp.where(lanes < BLOCK, mixed, lower)
    return jnp.concatenate([body, jnp.broadcast_to(diagonal, (8, PAIR))], axis=0)


def unpacked(packed):
    rows = lax.broadcasted_iota(jnp.int32, (BLOCK, PAIR), 0)
    lanes = lax.broadcasted_iota(jnp.int32, (BLOCK, PAIR), 1)
    columns = jnp.where(lanes < BLOCK, lanes, lanes - BLOCK)
    body = packed[:BLOCK]
    flipped = jnp.concatenate([body, body], axis=0).T
    mixed_t, lower_t = flipped[:BLOCK], flipped[BLOCK:]
    moved = pltpu.roll(body, BLOCK, 1)
    top = jnp.where(lanes < BLOCK, jnp.where(rows > columns, mixed_t, body), -lower_t)
    corner = jnp.where(rows == columns, packed[BLOCK : BLOCK + 1], jnp.where(rows > columns, moved, mixed_t))
    bottom = jnp.where(lanes < BLOCK, moved, corner)
    return jnp.concatenate([top, bottom], axis=0)


def gram_packed(block):
    high, low = split(block)
    lefts = jnp.concatenate([high[:BLOCK], low[:BLOCK]], axis=0)
    rights = jnp.concatenate([high[BLOCK:], low[BLOCK:]], axis=0)
    parts = product(lefts, rights, NT)
    halves = parts[:BLOCK] + parts[BLOCK:]
    cross = halves + pltpu.roll(halves, BLOCK, 1)
    lane = lax.broadcasted_iota(jnp.int32, (HALF, PAIR), 1)
    cross = jnp.where(lane < BLOCK, cross[:HALF], cross[HALF:])
    squares = block * block
    partial = squares[:, :128]
    for start in range(128, squares.shape[1], 128):
        partial = partial + squares[:, start : start + 128]
    norms = jnp.broadcast_to(jnp.sum(partial.T, axis=0, keepdims=True), (8, PAIR))
    rows = lax.broadcasted_iota(jnp.int32, (8, PAIR), 0)
    lanes = lax.broadcasted_iota(jnp.int32, (8, PAIR), 1)
    norms = jnp.where(jnp.logical_and(rows == 1, lanes < BLOCK), pltpu.roll(norms, BLOCK, 1), norms)
    return jnp.concatenate([cross, norms], axis=0)


def turned(packed, block):
    high, low = split(block)
    turn_high, turn_middle, turn_low = split3(unpacked(packed))
    lefts = jnp.concatenate([turn_high, turn_middle, turn_low, turn_high], axis=1)
    return product(lefts, jnp.concatenate([high, high, high, low], axis=0))


def kernel(rows, cols, pairs, order_ref, columns_ref, out_ref, raw, x0, x1, grams, parts, turns, edges,
           gram_send, gram_recv, turn_send, turn_recv, pass_send, edge_send, edge_recv, in_sem, out_sem):
    buffers = (x0, x1)
    arrival = pltpu.make_async_copy(columns_ref, raw, in_sem)
    arrival.start()
    me = lax.axis_index("row")
    position = lax.axis_index("col")
    core = lax.rem(me, 2)
    chip = lax.div(me, 2)
    partner = me + 1 - 2 * core
    has_left = position > 0
    has_right = position < cols - 1
    last = pairs - 1
    width = pairs * PAIR

    barrier = pltpu.get_barrier_semaphore()

    def greet(other, carry):
        @pl.when(other != me)
        def _():
            pl.semaphore_signal(barrier, inc=1, device_id={"row": other})
        return carry

    lax.fori_loop(0, rows, greet, 0)

    @pl.when(has_left)
    def _():
        pl.semaphore_signal(barrier, inc=1, device_id={"col": position - 1})

    @pl.when(has_right)
    def _():
        pl.semaphore_signal(barrier, inc=1, device_id={"col": position + 1})

    def fill(slot, carry):
        source = lax.rem(order_ref[slot], 2 * pairs)
        x0[pl.ds(pl.multiple_of(slot * BLOCK, BLOCK), BLOCK), :] = raw[source]
        return carry

    arrival.wait()
    lax.fori_loop(0, 2 * pairs, fill, 0)

    greeted = rows - 1 + has_left.astype(jnp.int32) + has_right.astype(jnp.int32)
    pl.semaphore_wait(barrier, greeted)

    def gram_copy(pair):
        return pltpu.make_async_remote_copy(
            src_ref=grams.at[pair], dst_ref=parts.at[me], send_sem=gram_send.at[pair], recv_sem=gram_recv.at[me],
            device_id={"row": pair},
        )

    def gram_arrival(source):
        return pltpu.make_async_remote_copy(
            src_ref=parts.at[source], dst_ref=parts.at[source], send_sem=gram_send.at[0],
            recv_sem=gram_recv.at[source], device_id={"row": partner},
        )

    def turn_copy(other):
        target = jnp.where(other == chip, partner, 2 * other + core)
        return pltpu.make_async_remote_copy(
            src_ref=turns.at[me], dst_ref=turns.at[me], send_sem=turn_send.at[other], recv_sem=turn_recv.at[me],
            device_id={"row": target},
        )

    def pass_copy(pair):
        return pltpu.make_async_remote_copy(
            src_ref=turns.at[pair], dst_ref=turns.at[pair], send_sem=pass_send.at[pair], recv_sem=turn_recv.at[pair],
            device_id={"row": partner},
        )

    def edge_left(after):
        return pltpu.make_async_remote_copy(
            src_ref=edges.at[0], dst_ref=buffers[after].at[pl.ds(last * PAIR + BLOCK, BLOCK)], send_sem=edge_send.at[0],
            recv_sem=edge_recv.at[after, 0], device_id={"col": position - 1},
        )

    def edge_right(after):
        return pltpu.make_async_remote_copy(
            src_ref=edges.at[1], dst_ref=buffers[after].at[pl.ds(0, BLOCK)], send_sem=edge_send.at[1],
            recv_sem=edge_recv.at[after, 1], device_id={"col": position + 1},
        )

    def wait_edges(now):
        @pl.when(has_left)
        def _():
            edge_right(now).wait_recv()

        @pl.when(has_right)
        def _():
            edge_left(now).wait_recv()

    def block_of(pair, now):
        return buffers[now][pl.ds(pl.multiple_of(pair * PAIR, PAIR), PAIR), :]

    def take_grams(first, second, now):
        for pair in (first, second):
            grams[pair] = gram_packed(block_of(pair, now))
        for pair in (first, second):
            @pl.when(pair != me)
            def _(pair=pair):
                gram_copy(pair).start()

    def own():
        def gather(source, carry):
            @pl.when(source != me)
            def _():
                gram_arrival(source).wait_recv()
            return carry

        lax.fori_loop(0, rows, gather, 0)
        total = grams[me]
        for source in range(rows):
            total = total + jnp.where(source == me, 0.0, parts[source])
        turns[me] = turn_packed(total)

        def spread_out(other, carry):
            turn_copy(other).start()
            return carry

        lax.fori_loop(0, rows // 2, spread_out, 0)

    def take_turn(pair):
        @pl.when(pair != me)
        def _():
            pass_copy(pair).wait_recv()

            @pl.when(lax.rem(pair, 2) == core)
            def _():
                pass_copy(pair).start()

    def step(index, now):
        after = 1 - now
        later = buffers[after]

        def inner_gram(group, carry):
            take_grams(2 * group + 1, 2 * group + 2, now)
            return carry

        lax.fori_loop(0, (pairs - 2) // 2, inner_gram, 0)

        @pl.when(index > 0)
        def _():
            wait_edges(now)

        take_grams(0, last, now)

        @pl.when(me < pairs)
        def _():
            own()

        @pl.when(jnp.logical_and(index > 0, has_left))
        def _():
            edge_left(after).wait_send()

        @pl.when(jnp.logical_and(index > 0, has_right))
        def _():
            edge_right(after).wait_send()

        take_turn(0)
        take_turn(last)
        first_turned = turned(turns[0], block_of(0, now))
        last_turned = turned(turns[last], block_of(last, now))
        later[pl.ds(pl.multiple_of(jnp.where(has_left, PAIR, 0), BLOCK), BLOCK), :] = first_turned[:BLOCK]
        edges[0] = first_turned[BLOCK:]
        edges[1] = last_turned[:BLOCK]
        later[pl.ds((last - 1) * PAIR + BLOCK, BLOCK), :] = last_turned[BLOCK:]

        @pl.when(has_left)
        def _():
            edge_left(after).start()

        @pl.when(jnp.logical_not(has_left))
        def _():
            later[pl.ds(PAIR, BLOCK), :] = edges[0]

        @pl.when(has_right)
        def _():
            edge_right(after).start()

        @pl.when(jnp.logical_not(has_right))
        def _():
            later[pl.ds(last * PAIR + BLOCK, BLOCK), :] = edges[1]

        def inner_apply(group, carry):
            chosen = (2 * group + 1, 2 * group + 2)
            for pair in chosen:
                take_turn(pair)
            for pair in chosen:
                result = turned(turns[pair], block_of(pair, now))
                later[pl.ds(pl.multiple_of((pair + 1) * PAIR, PAIR), BLOCK), :] = result[:BLOCK]
                later[pl.ds(pl.multiple_of((pair - 1) * PAIR + BLOCK, BLOCK), BLOCK), :] = result[BLOCK:]
            return carry

        lax.fori_loop(0, (pairs - 2) // 2, inner_apply, 0)

        def settle(pair, carry):
            @pl.when(pair != me)
            def _():
                gram_copy(pair).wait_send()

                @pl.when(lax.rem(pair, 2) == core)
                def _():
                    pass_copy(pair).wait_send()
            return carry

        lax.fori_loop(0, pairs, settle, 0)

        @pl.when(me < pairs)
        def _():
            def settle_turn(other, carry):
                turn_copy(other).wait_send()
                return carry

            lax.fori_loop(0, rows // 2, settle_turn, 0)

    def two_steps(index, carry):
        step(2 * index, 0)
        step(2 * index + 1, 1)
        return carry

    lax.fori_loop(0, STEPS // 2, two_steps, 0)
    final = STEPS % 2

    def out_copy(start, size, which):
        return pltpu.make_async_copy(
            buffers[final].at[pl.ds(start, size)], out_ref.at[pl.ds(start, size)], out_sem.at[which]
        )

    middle = out_copy(BLOCK, width - PAIR, 0)
    middle.start()
    wait_edges(final)
    first = out_copy(0, BLOCK, 1)
    first.start()
    ending = out_copy(width - BLOCK, BLOCK, 2)
    ending.start()

    @pl.when(has_left)
    def _():
        edge_left(final).wait_send()

    @pl.when(has_right)
    def _():
        edge_right(final).wait_send()

    middle.wait()
    first.wait()
    ending.wait()


def solution(mesh):
    rows, cols = mesh.shape["row"], mesh.shape["col"]

    def local(columns, block_order):
        width, length = columns.shape
        pairs = width // PAIR
        assert 4 <= pairs <= rows and rows % 2 == 0 and pairs % 2 == 0
        dma = pltpu.SemaphoreType.DMA
        return pl.pallas_call(
            functools.partial(kernel, rows, cols, pairs),
            out_shape=jax.ShapeDtypeStruct((width, length), jnp.float32),
            in_specs=[pl.BlockSpec(memory_space=pltpu.SMEM), pl.BlockSpec(memory_space=pl.ANY)],
            out_specs=pl.BlockSpec(memory_space=pl.ANY),
            scratch_shapes=[
                pltpu.VMEM((2 * pairs, BLOCK, length), jnp.float32),
                pltpu.VMEM((width, length), jnp.float32),
                pltpu.VMEM((width, length), jnp.float32),
                pltpu.VMEM((pairs, PACKED, PAIR), jnp.float32),
                pltpu.VMEM((rows, PACKED, PAIR), jnp.float32),
                pltpu.VMEM((pairs, BLOCK + 8, PAIR), jnp.float32),
                pltpu.VMEM((2, BLOCK, length), jnp.float32),
                dma((pairs,)),
                dma((rows,)),
                dma((rows // 2,)),
                dma((pairs,)),
                dma((pairs,)),
                dma((2,)),
                dma((2, 2)),
                dma,
                dma((3,)),
            ],
            compiler_params=pltpu.CompilerParams(
                collective_id=0, has_side_effects=True, vmem_limit_bytes=56 * 1024 * 1024
            ),
        )(block_order, columns.reshape(2 * pairs, BLOCK, length))

    placed = (P("col", "row"), P("col"))
    return jax.shard_map(local, mesh=mesh, in_specs=placed, out_specs=P("col", "row"), check_vma=False)
```

```python
import functools

import jax
import jax.numpy as jnp
from jax import lax
from jax.experimental import pallas as pl
from jax.experimental.pallas import tpu as pltpu
from jax.sharding import PartitionSpec as P

BLOCK = 64
PAIR = 2 * BLOCK
STEPS = 4
HALF = BLOCK // 2
PACKED = HALF + 8
UPPER = 1.0 + BLOCK * BLOCK * 0.0905
NN = (((1,), (0,)), ((), ()))
NT = (((1,), (1,)), ((), ()))


def split(a):
    high = a.astype(jnp.bfloat16)
    return high, (a - high.astype(jnp.float32)).astype(jnp.bfloat16)


def split3(a):
    high = a.astype(jnp.bfloat16)
    rest = a - high.astype(jnp.float32)
    middle = rest.astype(jnp.bfloat16)
    return high, middle, (rest - middle.astype(jnp.float32)).astype(jnp.bfloat16)


def product(a, b, dims=NN):
    return lax.dot_general(a, b, dims, preferred_element_type=jnp.float32)


def mm3(a, b):
    (ah, am), (bh, bm) = split(a), split(b)
    count = a.shape[0]
    stacked = product(jnp.concatenate([ah, am], axis=0), bh)
    return stacked[:count] + stacked[count:] + product(ah, bm)


def mm6(a, b, dims=NN):
    (ah, am, al), (bh, bm, bl) = split3(a), split3(b)
    count = a.shape[0]
    first = product(jnp.concatenate([ah, am, al], axis=0), bh, dims)
    second = product(jnp.concatenate([ah, am], axis=0), bm, dims)
    small = first[2 * count :] + second[count:] + product(ah, bl, dims)
    return first[:count] + ((first[count : 2 * count] + second[:count]) + small)


def left(a):
    return a[:, :BLOCK]


def inverse(system, eye):
    low = 2.0 / (1.0 + UPPER)
    y = system * low
    reach = low * (2.0 - low)
    scale = 2.0 / (1.0 + reach)
    x = (scale * low) * (2.0 * eye - y)
    y = scale * (2.0 * y - mm3(left(y), y))
    low = scale * reach
    while low < 0.999:
        reach = low * (2.0 - low)
        scale = 2.0 / (1.0 + reach)
        following = scale * (2.0 * y - mm3(left(y), y))
        x = scale * (2.0 * x - mm3(left(x), y))
        y = following
        low = scale * reach
    return x


def turn_packed(total):
    row = lax.broadcasted_iota(jnp.int32, (HALF, PAIR), 0)
    lane = lax.broadcasted_iota(jnp.int32, (HALF, PAIR), 1)
    cross = total[:HALF]
    norms = total[HALF : HALF + 1]
    bottom_norms = total[HALF + 1 : HALF + 2]
    upper_norms = jnp.sum(jnp.where(lane == row, norms, 0.0), axis=1, keepdims=True)
    lower_norms = jnp.sum(jnp.where(lane == row + HALF, norms, 0.0), axis=1, keepdims=True)
    top_norms = jnp.where(lane < BLOCK, upper_norms, lower_norms)
    spread = bottom_norms - top_norms
    square = spread * spread + 4.0 * cross * cross
    radius = jnp.sqrt(square)
    scale_term = (top_norms + bottom_norms) / BLOCK
    packed = 2.0 * cross * spread / (square + jnp.abs(spread) * radius + scale_term * scale_term)
    rolled = pltpu.roll(packed, BLOCK, 1)
    coupling = jnp.concatenate([jnp.where(lane < BLOCK, packed, rolled), jnp.where(lane < BLOCK, rolled, packed)], axis=0)
    rows = lax.broadcasted_iota(jnp.int32, (BLOCK, PAIR), 0)
    lanes = lax.broadcasted_iota(jnp.int32, (BLOCK, PAIR), 1)
    columns = jnp.where(lanes < BLOCK, lanes, lanes - BLOCK)
    eye = jnp.where(rows == columns, 1.0, 0.0).astype(jnp.float32)
    narrow = left(coupling)
    narrow_t = narrow.T
    system = eye + mm6(narrow, jnp.concatenate([narrow, narrow], axis=0), NT)
    x = inverse(system, eye)
    lower = mm6(narrow_t, x)
    residual = eye - x - mm6(narrow, lower)
    stacked = jnp.concatenate([x, lower], axis=0)
    stacked = stacked + mm3(left(stacked), residual)
    x, lower = stacked[:BLOCK], 2.0 * stacked[BLOCK:]
    corner = eye - mm6(left(lower), coupling)
    diagonal = jnp.sum(jnp.where(rows == columns, corner, 0.0), axis=0, keepdims=True)
    mixed = jnp.where(rows <= columns, 2.0 * x - eye, corner)
    body = jnp.where(lanes < BLOCK, mixed, lower)
    return jnp.concatenate([body, jnp.broadcast_to(diagonal, (8, PAIR))], axis=0)


def unpacked(packed):
    rows = lax.broadcasted_iota(jnp.int32, (BLOCK, PAIR), 0)
    lanes = lax.broadcasted_iota(jnp.int32, (BLOCK, PAIR), 1)
    columns = jnp.where(lanes < BLOCK, lanes, lanes - BLOCK)
    body = packed[:BLOCK]
    flipped = jnp.concatenate([body, body], axis=0).T
    mixed_t, lower_t = flipped[:BLOCK], flipped[BLOCK:]
    moved = pltpu.roll(body, BLOCK, 1)
    top = jnp.where(lanes < BLOCK, jnp.where(rows > columns, mixed_t, body), -lower_t)
    corner = jnp.where(rows == columns, packed[BLOCK : BLOCK + 1], jnp.where(rows > columns, moved, mixed_t))
    bottom = jnp.where(lanes < BLOCK, moved, corner)
    return jnp.concatenate([top, bottom], axis=0)


def gram_packed(block):
    high, low = split(block)
    lefts = jnp.concatenate([high[:BLOCK], low[:BLOCK]], axis=0)
    rights = jnp.concatenate([high[BLOCK:], low[BLOCK:]], axis=0)
    parts = product(lefts, rights, NT)
    halves = parts[:BLOCK] + parts[BLOCK:]
    cross = halves + pltpu.roll(halves, BLOCK, 1)
    lane = lax.broadcasted_iota(jnp.int32, (HALF, PAIR), 1)
    cross = jnp.where(lane < BLOCK, cross[:HALF], cross[HALF:])
    squares = block * block
    partial = squares[:, :128]
    for start in range(128, squares.shape[1], 128):
        partial = partial + squares[:, start : start + 128]
    norms = jnp.broadcast_to(jnp.sum(partial.T, axis=0, keepdims=True), (8, PAIR))
    rows = lax.broadcasted_iota(jnp.int32, (8, PAIR), 0)
    lanes = lax.broadcasted_iota(jnp.int32, (8, PAIR), 1)
    norms = jnp.where(jnp.logical_and(rows == 1, lanes < BLOCK), pltpu.roll(norms, BLOCK, 1), norms)
    return jnp.concatenate([cross, norms], axis=0)


def apply_turn(matrix, block):
    high, low = split(block)
    turn_high, turn_middle, turn_low = split3(matrix)
    lefts = jnp.concatenate([turn_high, turn_middle, turn_low, turn_high], axis=1)
    return product(lefts, jnp.concatenate([high, high, high, low], axis=0))


def turned(packed, block):
    return apply_turn(unpacked(packed), block)


def turned_half(packed, block, side):
    matrix = unpacked(packed)
    return apply_turn(matrix[:BLOCK] if side == 0 else matrix[BLOCK:], block)


def kernel(rows, cols, pairs, order_ref, columns_ref, out_ref, raw, x0, x1, grams, parts, turns, halos,
           gram_send, gram_recv, turn_send, turn_recv, pass_send, halo_send, halo_recv, relay_send,
           start_send, start_recv, edge_send, edge_recv, in_sem, out_sem):
    buffers = (x0, x1)
    arrival = pltpu.make_async_copy(columns_ref, raw, in_sem)
    arrival.start()
    me = lax.axis_index("row")
    position = lax.axis_index("col")
    core = lax.rem(me, 2)
    chip = lax.div(me, 2)
    partner = me + 1 - 2 * core
    base = lax.rem(me, pairs)
    has_left = position > 0
    has_right = position < cols - 1
    has = (has_left, has_right)
    beside = (position - 1, position + 1)
    last = pairs - 1
    direct = (last % 2, 0)
    half = rows // 2

    barrier = pltpu.get_barrier_semaphore()

    def greet(other, carry):
        @pl.when(other != me)
        def _():
            pl.semaphore_signal(barrier, inc=1, device_id={"row": other})

        for side in (0, 1):
            @pl.when(has[side])
            def _(side=side):
                pl.semaphore_signal(barrier, inc=1, device_id={"row": other, "col": beside[side]})
        return carry

    lax.fori_loop(0, rows, greet, 0)

    def fill(slot, carry):
        source = lax.rem(order_ref[slot], 2 * pairs)
        x0[pl.ds(pl.multiple_of(slot * BLOCK + PAIR, BLOCK), BLOCK), :] = raw[source]
        return carry

    arrival.wait()
    lax.fori_loop(0, 2 * pairs, fill, 0)
    greeted = rows - 1 + rows * (has_left.astype(jnp.int32) + has_right.astype(jnp.int32))
    pl.semaphore_wait(barrier, greeted)

    def gram_copy(pair):
        return pltpu.make_async_remote_copy(
            src_ref=grams.at[pair], dst_ref=parts.at[me], send_sem=gram_send.at[pair], recv_sem=gram_recv.at[me],
            device_id={"row": pair},
        )

    def gram_arrival(source):
        return pltpu.make_async_remote_copy(
            src_ref=parts.at[source], dst_ref=parts.at[source], send_sem=gram_send.at[0],
            recv_sem=gram_recv.at[source], device_id={"row": partner},
        )

    def turn_copy(other):
        target = jnp.where(other == chip, partner, 2 * other + core)
        return pltpu.make_async_remote_copy(
            src_ref=turns.at[me], dst_ref=turns.at[me], send_sem=turn_send.at[other], recv_sem=turn_recv.at[me],
            device_id={"row": target},
        )

    def pass_copy(pair):
        return pltpu.make_async_remote_copy(
            src_ref=turns.at[pair], dst_ref=turns.at[pair], send_sem=pass_send.at[pair], recv_sem=turn_recv.at[pair],
            device_id={"row": partner},
        )

    def halo_copy(other, side, now):
        return pltpu.make_async_remote_copy(
            src_ref=turns.at[me], dst_ref=halos.at[now, side], send_sem=halo_send.at[other],
            recv_sem=halo_recv.at[now, side], device_id={"row": 2 * other + core, "col": beside[1 - side]},
        )

    def relay_copy(side, now):
        return pltpu.make_async_remote_copy(
            src_ref=halos.at[now, side], dst_ref=halos.at[now, side], send_sem=relay_send.at[side],
            recv_sem=halo_recv.at[now, side], device_id={"row": partner},
        )

    far = (pairs + 1) * PAIR

    def start_copy(side):
        source = pairs * PAIR if side == 0 else PAIR
        target = 0 if side == 0 else far
        return pltpu.make_async_remote_copy(
            src_ref=x0.at[pl.ds(source, PAIR)], dst_ref=x0.at[pl.ds(target, PAIR)], send_sem=start_send.at[side],
            recv_sem=start_recv.at[side], device_id={"col": beside[1 - side]},
        )

    def edge_copy(side, after):
        source = pairs * PAIR if side == 0 else PAIR + BLOCK
        target = 0 if side == 0 else far + BLOCK
        return pltpu.make_async_remote_copy(
            src_ref=buffers[after].at[pl.ds(source, BLOCK)], dst_ref=buffers[after].at[pl.ds(target, BLOCK)],
            send_sem=edge_send.at[after, side], recv_sem=edge_recv.at[after, side],
            device_id={"col": beside[1 - side]},
        )

    for side in (0, 1):
        @pl.when(has[1 - side])
        def _(side=side):
            start_copy(side).start()

    def slot_of(slot, now):
        return buffers[now][pl.ds(pl.multiple_of(slot * PAIR, PAIR), PAIR), :]

    def own():
        def gather(source, carry):
            @pl.when(source != me)
            def _():
                gram_arrival(source).wait_recv()
            return carry

        lax.fori_loop(0, rows, gather, 0)
        total = grams[me]
        for source in range(rows):
            total = total + jnp.where(source == me, 0.0, parts[source])
        turns[me] = turn_packed(total)

    def step(index, now):
        after = 1 - now
        later = buffers[after]

        def take_grams(group, carry):
            chosen = (2 * group, 2 * group + 1)
            for pair in chosen:
                grams[pair] = gram_packed(slot_of(pair + 1, now))
            for pair in chosen:
                @pl.when(pair != me)
                def _(pair=pair):
                    gram_copy(pair).start()
            return carry

        lax.fori_loop(0, pairs // 2, take_grams, 0)

        @pl.when(me < pairs)
        def _():
            own()

            def spread_out(other, carry):
                turn_copy(other).start()
                return carry

            lax.fori_loop(0, half, spread_out, 0)

        for side, owner in ((0, last), (1, 0)):
            @pl.when(jnp.logical_and(me == owner, has[1 - side]))
            def _(side=side):
                def spread_halo(other, carry):
                    halo_copy(other, side, now).start()
                    return carry

                lax.fori_loop(0, half, spread_halo, 0)

        @pl.when(index > 1)
        def _():
            for side in (0, 1):
                @pl.when(has[1 - side])
                def _(side=side):
                    edge_copy(side, after).wait_send()

        if now == 1:
            @pl.when(index == 1)
            def _():
                for side in (0, 1):
                    @pl.when(has[1 - side])
                    def _(side=side):
                        start_copy(side).wait_send()

        def receive(pair):
            @pl.when(pair != me)
            def _():
                pass_copy(pair).wait_recv()

                @pl.when(lax.rem(pair, 2) == core)
                def _():
                    pass_copy(pair).start()

        def receive_halo(side):
            @pl.when(has[side])
            def _():
                relay_copy(side, now).wait_recv()

                @pl.when(core == direct[side])
                def _():
                    relay_copy(side, now).start()

        def pair_at(place):
            even = 2 * (place - 1)
            odd = 2 * (place - pairs // 2) + 1
            shift = jnp.where(place < 2, place, jnp.where(place <= pairs // 2, even, odd))
            return jnp.bitwise_xor(base, shift)

        def apply_two(first, second):
            results = [turned(turns[pair], slot_of(pair + 1, now)) for pair in (first, second)]
            for pair, result in zip((first, second), results):
                opening = jnp.logical_and(pair == 0, jnp.logical_not(has_left))
                closing = jnp.logical_and(pair == last, jnp.logical_not(has_right))
                top = jnp.where(opening, PAIR, jnp.where(closing, pairs * PAIR + BLOCK, (pair + 2) * PAIR))
                bottom = jnp.where(opening, 2 * PAIR, pair * PAIR + BLOCK)
                later[pl.ds(pl.multiple_of(top, BLOCK), BLOCK), :] = result[:BLOCK]
                later[pl.ds(pl.multiple_of(bottom, BLOCK), BLOCK), :] = result[BLOCK:]

        receive(pair_at(0))
        receive(pair_at(1))
        apply_two(pair_at(0), pair_at(1))

        def receive_direct(place, carry):
            receive(pair_at(place))
            return carry

        lax.fori_loop(2, pairs // 2 + 1, receive_direct, 0)
        for side in (0, 1):
            @pl.when(core == direct[side])
            def _(side=side):
                receive_halo(side)

        def apply_rest(group, carry):
            for place in (2 * group, 2 * group + 1):
                @pl.when(place > pairs // 2)
                def _(place=place):
                    receive(pair_at(place))
            apply_two(pair_at(2 * group), pair_at(2 * group + 1))
            return carry

        lax.fori_loop(1, pairs // 2, apply_rest, 0)
        for side in (0, 1):
            @pl.when(core != direct[side])
            def _(side=side):
                receive_halo(side)

        for side in (0, 1):
            @pl.when(has[side])
            def _(side=side):
                if now == 0:
                    @pl.when(index == 0)
                    def _():
                        start_copy(side).wait_recv()

                    @pl.when(index > 0)
                    def _():
                        edge_copy(side, now).wait_recv()
                else:
                    edge_copy(side, now).wait_recv()
                rest = turned_half(halos[now, side], slot_of(side * (pairs + 1), now), side)
                target = PAIR if side == 0 else pairs * PAIR + BLOCK
                later[pl.ds(target, BLOCK), :] = rest

        @pl.when(index < STEPS - 1)
        def _():
            for side in (0, 1):
                @pl.when(has[1 - side])
                def _(side=side):
                    edge_copy(side, after).start()

        def settle(pair, carry):
            @pl.when(pair != me)
            def _():
                gram_copy(pair).wait_send()

                @pl.when(lax.rem(pair, 2) == core)
                def _():
                    pass_copy(pair).wait_send()
            return carry

        lax.fori_loop(0, pairs, settle, 0)

        @pl.when(me < pairs)
        def _():
            def settle_turn(other, carry):
                turn_copy(other).wait_send()
                return carry

            lax.fori_loop(0, half, settle_turn, 0)

        for side, owner in ((0, last), (1, 0)):
            @pl.when(jnp.logical_and(me == owner, has[1 - side]))
            def _(side=side):
                def settle_halo(other, carry):
                    halo_copy(other, side, now).wait_send()
                    return carry

                lax.fori_loop(0, half, settle_halo, 0)

            @pl.when(jnp.logical_and(core == direct[side], has[side]))
            def _(side=side):
                relay_copy(side, now).wait_send()

    def two_steps(index, carry):
        step(2 * index, 0)
        step(2 * index + 1, 1)
        return carry

    lax.fori_loop(0, STEPS // 2, two_steps, 0)
    final = STEPS % 2
    result = pltpu.make_async_copy(buffers[final].at[pl.ds(PAIR, pairs * PAIR)], out_ref, out_sem)
    result.start()
    for side in (0, 1):
        @pl.when(has[1 - side])
        def _(side=side):
            edge_copy(side, 1 - final).wait_send()

    result.wait()


def solution(mesh):
    rows, cols = mesh.shape["row"], mesh.shape["col"]

    def local(columns, block_order):
        width, length = columns.shape
        pairs = width // PAIR
        assert 4 <= pairs <= rows and rows % pairs == 0 and pairs & (pairs - 1) == 0 and STEPS % 2 == 0
        dma = pltpu.SemaphoreType.DMA
        buffer = pltpu.VMEM((width + 2 * PAIR, length), jnp.float32)
        return pl.pallas_call(
            functools.partial(kernel, rows, cols, pairs),
            out_shape=jax.ShapeDtypeStruct((width, length), jnp.float32),
            in_specs=[pl.BlockSpec(memory_space=pltpu.SMEM), pl.BlockSpec(memory_space=pl.ANY)],
            out_specs=pl.BlockSpec(memory_space=pl.ANY),
            scratch_shapes=[
                pltpu.VMEM((2 * pairs, BLOCK, length), jnp.float32),
                buffer,
                buffer,
                pltpu.VMEM((pairs, PACKED, PAIR), jnp.float32),
                pltpu.VMEM((rows, PACKED, PAIR), jnp.float32),
                pltpu.VMEM((pairs, BLOCK + 8, PAIR), jnp.float32),
                pltpu.VMEM((2, 2, BLOCK + 8, PAIR), jnp.float32),
                dma((pairs,)),
                dma((rows,)),
                dma((rows // 2,)),
                dma((pairs,)),
                dma((pairs,)),
                dma((rows // 2,)),
                dma((2, 2)),
                dma((2,)),
                dma((2,)),
                dma((2,)),
                dma((2, 2)),
                dma((2, 2)),
                dma,
                dma,
            ],
            compiler_params=pltpu.CompilerParams(
                collective_id=0, has_side_effects=True, vmem_limit_bytes=56 * 1024 * 1024
            ),
        )(block_order, columns.reshape(2 * pairs, BLOCK, length))

    placed = (P("col", "row"), P("col"))
    return jax.shard_map(local, mesh=mesh, in_specs=placed, out_specs=P("col", "row"), check_vma=False)
```

```python
import functools

import jax
import jax.numpy as jnp
from jax import lax
from jax.experimental import pallas as pl
from jax.experimental.pallas import tpu as pltpu
from jax.sharding import PartitionSpec as P

BLOCK = 64
PAIR = 2 * BLOCK
STEPS = 4
HALF = BLOCK // 2
PACKED = HALF + 8
UPPER = 1.0 + BLOCK * BLOCK * 0.0905
NN = (((1,), (0,)), ((), ()))
NT = (((1,), (1,)), ((), ()))


def split(a):
    high = a.astype(jnp.bfloat16)
    return high, (a - high.astype(jnp.float32)).astype(jnp.bfloat16)


def split3(a):
    high = a.astype(jnp.bfloat16)
    rest = a - high.astype(jnp.float32)
    middle = rest.astype(jnp.bfloat16)
    return high, middle, (rest - middle.astype(jnp.float32)).astype(jnp.bfloat16)


def product(a, b, dims=NN):
    return lax.dot_general(a, b, dims, preferred_element_type=jnp.float32)


def mm3(a, b):
    (ah, am), (bh, bm) = split(a), split(b)
    count = a.shape[0]
    stacked = product(jnp.concatenate([ah, am], axis=0), bh)
    return stacked[:count] + stacked[count:] + product(ah, bm)


def mm6(a, b, dims=NN):
    (ah, am, al), (bh, bm, bl) = split3(a), split3(b)
    count = a.shape[0]
    first = product(jnp.concatenate([ah, am, al], axis=0), bh, dims)
    second = product(jnp.concatenate([ah, am], axis=0), bm, dims)
    small = first[2 * count :] + second[count:] + product(ah, bl, dims)
    return first[:count] + ((first[count : 2 * count] + second[:count]) + small)


def left(a):
    return a[:, :BLOCK]


def inverse(system, eye):
    low = 2.0 / (1.0 + UPPER)
    y = system * low
    reach = low * (2.0 - low)
    scale = 2.0 / (1.0 + reach)
    x = (scale * low) * (2.0 * eye - y)
    y = scale * (2.0 * y - mm3(left(y), y))
    low = scale * reach
    while low < 0.999:
        reach = low * (2.0 - low)
        scale = 2.0 / (1.0 + reach)
        following = scale * (2.0 * y - mm3(left(y), y))
        x = scale * (2.0 * x - mm3(left(x), y))
        y = following
        low = scale * reach
    return x


def turn_packed(total):
    row = lax.broadcasted_iota(jnp.int32, (HALF, PAIR), 0)
    lane = lax.broadcasted_iota(jnp.int32, (HALF, PAIR), 1)
    cross = total[:HALF]
    norms = total[HALF : HALF + 1]
    bottom_norms = total[HALF + 1 : HALF + 2]
    upper_norms = jnp.sum(jnp.where(lane == row, norms, 0.0), axis=1, keepdims=True)
    lower_norms = jnp.sum(jnp.where(lane == row + HALF, norms, 0.0), axis=1, keepdims=True)
    top_norms = jnp.where(lane < BLOCK, upper_norms, lower_norms)
    spread = bottom_norms - top_norms
    square = spread * spread + 4.0 * cross * cross
    radius = jnp.sqrt(square)
    scale_term = (top_norms + bottom_norms) / BLOCK
    packed = 2.0 * cross * spread / (square + jnp.abs(spread) * radius + scale_term * scale_term)
    rolled = pltpu.roll(packed, BLOCK, 1)
    coupling = jnp.concatenate([jnp.where(lane < BLOCK, packed, rolled), jnp.where(lane < BLOCK, rolled, packed)], axis=0)
    rows = lax.broadcasted_iota(jnp.int32, (BLOCK, PAIR), 0)
    lanes = lax.broadcasted_iota(jnp.int32, (BLOCK, PAIR), 1)
    columns = jnp.where(lanes < BLOCK, lanes, lanes - BLOCK)
    eye = jnp.where(rows == columns, 1.0, 0.0).astype(jnp.float32)
    narrow = left(coupling)
    narrow_t = narrow.T
    system = eye + mm6(narrow, jnp.concatenate([narrow, narrow], axis=0), NT)
    x = inverse(system, eye)
    lower = mm6(narrow_t, x)
    residual = eye - x - mm6(narrow, lower)
    stacked = jnp.concatenate([x, lower], axis=0)
    stacked = stacked + mm3(left(stacked), residual)
    x, lower = stacked[:BLOCK], 2.0 * stacked[BLOCK:]
    corner = eye - mm6(left(lower), coupling)
    diagonal = jnp.sum(jnp.where(rows == columns, corner, 0.0), axis=0, keepdims=True)
    mixed = jnp.where(rows <= columns, 2.0 * x - eye, corner)
    body = jnp.where(lanes < BLOCK, mixed, lower)
    return jnp.concatenate([body, jnp.broadcast_to(diagonal, (8, PAIR))], axis=0)


def unpacked(packed):
    rows = lax.broadcasted_iota(jnp.int32, (BLOCK, PAIR), 0)
    lanes = lax.broadcasted_iota(jnp.int32, (BLOCK, PAIR), 1)
    columns = jnp.where(lanes < BLOCK, lanes, lanes - BLOCK)
    body = packed[:BLOCK]
    flipped = jnp.concatenate([body, body], axis=0).T
    mixed_t, lower_t = flipped[:BLOCK], flipped[BLOCK:]
    moved = pltpu.roll(body, BLOCK, 1)
    top = jnp.where(lanes < BLOCK, jnp.where(rows > columns, mixed_t, body), -lower_t)
    corner = jnp.where(rows == columns, packed[BLOCK : BLOCK + 1], jnp.where(rows > columns, moved, mixed_t))
    bottom = jnp.where(lanes < BLOCK, moved, corner)
    return jnp.concatenate([top, bottom], axis=0)


def gram_packed(block):
    high, low = split(block)
    lefts = jnp.concatenate([high[:BLOCK], low[:BLOCK]], axis=0)
    rights = jnp.concatenate([high[BLOCK:], low[BLOCK:]], axis=0)
    parts = product(lefts, rights, NT)
    halves = parts[:BLOCK] + parts[BLOCK:]
    cross = halves + pltpu.roll(halves, BLOCK, 1)
    lane = lax.broadcasted_iota(jnp.int32, (HALF, PAIR), 1)
    cross = jnp.where(lane < BLOCK, cross[:HALF], cross[HALF:])
    squares = block * block
    partial = squares[:, :128]
    for start in range(128, squares.shape[1], 128):
        partial = partial + squares[:, start : start + 128]
    norms = jnp.broadcast_to(jnp.sum(partial.T, axis=0, keepdims=True), (8, PAIR))
    rows = lax.broadcasted_iota(jnp.int32, (8, PAIR), 0)
    lanes = lax.broadcasted_iota(jnp.int32, (8, PAIR), 1)
    norms = jnp.where(jnp.logical_and(rows == 1, lanes < BLOCK), pltpu.roll(norms, BLOCK, 1), norms)
    return jnp.concatenate([cross, norms], axis=0)


def apply_turn(matrix, block):
    high, low = split(block)
    turn_high, turn_middle, turn_low = split3(matrix)
    lefts = jnp.concatenate([turn_high, turn_middle, turn_low, turn_high], axis=1)
    return product(lefts, jnp.concatenate([high, high, high, low], axis=0))


def turned(packed, block):
    return apply_turn(unpacked(packed), block)


def turned_half(packed, block, side):
    matrix = unpacked(packed)
    return apply_turn(matrix[:BLOCK] if side == 0 else matrix[BLOCK:], block)


def kernel(rows, cols, pairs, order_ref, columns_ref, out_ref, raw, x0, x1, grams, parts, turns, halos,
           gram_send, gram_recv, turn_send, turn_recv, pass_send, halo_send, halo_recv, relay_send,
           start_send, start_recv, edge_send, edge_recv, in_sem, out_sem):
    buffers = (x0, x1)
    arrival = pltpu.make_async_copy(columns_ref, raw, in_sem)
    arrival.start()
    me = lax.axis_index("row")
    position = lax.axis_index("col")
    core = lax.rem(me, 2)
    chip = lax.div(me, 2)
    partner = me + 1 - 2 * core
    has_left = position > 0
    has_right = position < cols - 1
    has = (has_left, has_right)
    beside = (position - 1, position + 1)
    last = pairs - 1
    direct = (last % 2, 0)
    half = rows // 2

    barrier = pltpu.get_barrier_semaphore()

    def greet(other, carry):
        @pl.when(other != me)
        def _():
            pl.semaphore_signal(barrier, inc=1, device_id={"row": other})

        for side in (0, 1):
            @pl.when(has[side])
            def _(side=side):
                pl.semaphore_signal(barrier, inc=1, device_id={"row": other, "col": beside[side]})
        return carry

    lax.fori_loop(0, rows, greet, 0)

    def fill(pair):
        for slot in (2 * pair, 2 * pair + 1):
            source = lax.rem(order_ref[slot], 2 * pairs)
            x0[pl.ds(pl.multiple_of(slot * BLOCK + PAIR, BLOCK), BLOCK), :] = raw[source]

    def group_at(place):
        return pairs // 2 - 1 - place, pairs // 2 + place

    arrival.wait()
    fill(0)
    fill(last)
    greeted = rows - 1 + rows * (has_left.astype(jnp.int32) + has_right.astype(jnp.int32))
    pl.semaphore_wait(barrier, greeted)

    def gram_copy(pair):
        return pltpu.make_async_remote_copy(
            src_ref=grams.at[pair], dst_ref=parts.at[me], send_sem=gram_send.at[pair], recv_sem=gram_recv.at[me],
            device_id={"row": pair},
        )

    def gram_arrival(source):
        return pltpu.make_async_remote_copy(
            src_ref=parts.at[source], dst_ref=parts.at[source], send_sem=gram_send.at[0],
            recv_sem=gram_recv.at[source], device_id={"row": partner},
        )

    def turn_copy(other):
        target = jnp.where(other == chip, partner, 2 * other + core)
        return pltpu.make_async_remote_copy(
            src_ref=turns.at[me], dst_ref=turns.at[me], send_sem=turn_send.at[other], recv_sem=turn_recv.at[me],
            device_id={"row": target},
        )

    def pass_copy(pair):
        return pltpu.make_async_remote_copy(
            src_ref=turns.at[pair], dst_ref=turns.at[pair], send_sem=pass_send.at[pair], recv_sem=turn_recv.at[pair],
            device_id={"row": partner},
        )

    def halo_copy(other, side, now):
        return pltpu.make_async_remote_copy(
            src_ref=turns.at[me], dst_ref=halos.at[now, side], send_sem=halo_send.at[other],
            recv_sem=halo_recv.at[now, side], device_id={"row": 2 * other + core, "col": beside[1 - side]},
        )

    def relay_copy(side, now):
        return pltpu.make_async_remote_copy(
            src_ref=halos.at[now, side], dst_ref=halos.at[now, side], send_sem=relay_send.at[side],
            recv_sem=halo_recv.at[now, side], device_id={"row": partner},
        )

    far = (pairs + 1) * PAIR

    def start_copy(side):
        source = pairs * PAIR if side == 0 else PAIR
        target = 0 if side == 0 else far
        return pltpu.make_async_remote_copy(
            src_ref=x0.at[pl.ds(source, PAIR)], dst_ref=x0.at[pl.ds(target, PAIR)], send_sem=start_send.at[side],
            recv_sem=start_recv.at[side], device_id={"col": beside[1 - side]},
        )

    def edge_copy(side, after):
        source = pairs * PAIR if side == 0 else PAIR + BLOCK
        target = 0 if side == 0 else far + BLOCK
        return pltpu.make_async_remote_copy(
            src_ref=buffers[after].at[pl.ds(source, BLOCK)], dst_ref=buffers[after].at[pl.ds(target, BLOCK)],
            send_sem=edge_send.at[after, side], recv_sem=edge_recv.at[after, side],
            device_id={"col": beside[1 - side]},
        )

    for side in (0, 1):
        @pl.when(has[1 - side])
        def _(side=side):
            start_copy(side).start()

    def slot_of(slot, now):
        return buffers[now][pl.ds(pl.multiple_of(slot * PAIR, PAIR), PAIR), :]

    def own():
        def gather(source, carry):
            @pl.when(source != me)
            def _():
                gram_arrival(source).wait_recv()
            return carry

        lax.fori_loop(0, rows, gather, 0)
        total = grams[me]
        for source in range(rows):
            total = total + jnp.where(source == me, 0.0, parts[source])
        turns[me] = turn_packed(total)

    def take_grams(place, now):
        chosen = group_at(place)
        for pair in chosen:
            grams[pair] = gram_packed(slot_of(pair + 1, now))
        for pair in chosen:
            @pl.when(pair != me)
            def _(pair=pair):
                gram_copy(pair).start()

    def first_grams(place, carry):
        for pair in group_at(place):
            fill(pair)
        take_grams(place, 0)
        return carry

    lax.fori_loop(0, pairs // 2 - 1, first_grams, 0)
    take_grams(pairs // 2 - 1, 0)

    def step(index):
        now, after = index % 2, 1 - index % 2
        later = buffers[after]
        ending = index == STEPS - 1

        @pl.when(me < pairs)
        def _():
            own()

            def spread_out(other, carry):
                turn_copy(other).start()
                return carry

            lax.fori_loop(0, half, spread_out, 0)

        for side, owner in ((0, last), (1, 0)):
            @pl.when(jnp.logical_and(me == owner, has[1 - side]))
            def _(side=side):
                def spread_halo(other, carry):
                    halo_copy(other, side, now).start()
                    return carry

                lax.fori_loop(0, half, spread_halo, 0)

        def settle_gram(pair, carry):
            @pl.when(pair != me)
            def _():
                gram_copy(pair).wait_send()
            return carry

        lax.fori_loop(0, pairs, settle_gram, 0)

        for side in (0, 1):
            @pl.when(has[1 - side])
            def _(side=side):
                if index > 1:
                    edge_copy(side, after).wait_send()
                if index == 1:
                    start_copy(side).wait_send()

        def relay(pair):
            @pl.when(jnp.logical_and(pair != me, lax.rem(pair, 2) == core))
            def _():
                pass_copy(pair).wait_recv()
                pass_copy(pair).start()

        def receive_group(place):
            chosen = group_at(place)
            for pair in chosen:
                relay(pair)
            for pair in chosen:
                @pl.when(jnp.logical_and(pair != me, lax.rem(pair, 2) != core))
                def _(pair=pair):
                    pass_copy(pair).wait_recv()

        def settle_group(place):
            for pair in group_at(place):
                @pl.when(jnp.logical_and(pair != me, lax.rem(pair, 2) == core))
                def _(pair=pair):
                    pass_copy(pair).wait_send()

        def apply_group(place):
            chosen = group_at(place)
            results = [turned(turns[pair], slot_of(pair + 1, now)) for pair in chosen]
            for pair, result in zip(chosen, results):
                opening = jnp.logical_and(pair == 0, jnp.logical_not(has_left))
                closing = jnp.logical_and(pair == last, jnp.logical_not(has_right))
                top = jnp.where(opening, PAIR, jnp.where(closing, pairs * PAIR + BLOCK, (pair + 2) * PAIR))
                bottom = jnp.where(opening, 2 * PAIR, pair * PAIR + BLOCK)
                later[pl.ds(pl.multiple_of(top, BLOCK), BLOCK), :] = result[:BLOCK]
                later[pl.ds(pl.multiple_of(bottom, BLOCK), BLOCK), :] = result[BLOCK:]

        def next_grams(place):
            settle_group(place)
            if not ending:
                take_grams(place, after)

        receive_group(0)
        apply_group(0)

        def apply_next(place, carry):
            receive_group(place)
            apply_group(place)
            next_grams(place - 1)
            return carry

        lax.fori_loop(1, pairs // 2, apply_next, 0)

        def receive_halo(side):
            @pl.when(has[side])
            def _():
                relay_copy(side, now).wait_recv()

                @pl.when(core == direct[side])
                def _():
                    relay_copy(side, now).start()

        for relayed in (False, True):
            for side in (0, 1):
                @pl.when((core != direct[side]) == relayed)
                def _(side=side):
                    receive_halo(side)

        for side in (0, 1):
            @pl.when(has[side])
            def _(side=side):
                if index == 0:
                    start_copy(side).wait_recv()
                else:
                    edge_copy(side, now).wait_recv()
                rest = turned_half(halos[now, side], slot_of(side * (pairs + 1), now), side)
                target = PAIR if side == 0 else pairs * PAIR + BLOCK
                later[pl.ds(target, BLOCK), :] = rest

        next_grams(pairs // 2 - 1)
        for side in (0, 1):
            @pl.when(jnp.logical_and(core == direct[side], has[side]))
            def _(side=side):
                relay_copy(side, now).wait_send()

        if not ending:
            for side in (0, 1):
                @pl.when(has[1 - side])
                def _(side=side):
                    edge_copy(side, after).start()

        @pl.when(me < pairs)
        def _():
            def settle_turn(other, carry):
                turn_copy(other).wait_send()
                return carry

            lax.fori_loop(0, half, settle_turn, 0)

        for side, owner in ((0, last), (1, 0)):
            @pl.when(jnp.logical_and(me == owner, has[1 - side]))
            def _(side=side):
                def settle_halo(other, carry):
                    halo_copy(other, side, now).wait_send()
                    return carry

                lax.fori_loop(0, half, settle_halo, 0)

    for index in range(STEPS):
        step(index)
    final = STEPS % 2
    result = pltpu.make_async_copy(buffers[final].at[pl.ds(PAIR, pairs * PAIR)], out_ref, out_sem)
    result.start()
    for side in (0, 1):
        @pl.when(has[1 - side])
        def _(side=side):
            edge_copy(side, 1 - final).wait_send()

    result.wait()


def solution(mesh):
    rows, cols = mesh.shape["row"], mesh.shape["col"]

    def local(columns, block_order):
        width, length = columns.shape
        pairs = width // PAIR
        assert 4 <= pairs <= rows and rows % pairs == 0 and pairs & (pairs - 1) == 0 and STEPS % 2 == 0
        dma = pltpu.SemaphoreType.DMA
        buffer = pltpu.VMEM((width + 2 * PAIR, length), jnp.float32)
        return pl.pallas_call(
            functools.partial(kernel, rows, cols, pairs),
            out_shape=jax.ShapeDtypeStruct((width, length), jnp.float32),
            in_specs=[pl.BlockSpec(memory_space=pltpu.SMEM), pl.BlockSpec(memory_space=pl.ANY)],
            out_specs=pl.BlockSpec(memory_space=pl.ANY),
            scratch_shapes=[
                pltpu.VMEM((2 * pairs, BLOCK, length), jnp.float32),
                buffer,
                buffer,
                pltpu.VMEM((pairs, PACKED, PAIR), jnp.float32),
                pltpu.VMEM((rows, PACKED, PAIR), jnp.float32),
                pltpu.VMEM((pairs, BLOCK + 8, PAIR), jnp.float32),
                pltpu.VMEM((2, 2, BLOCK + 8, PAIR), jnp.float32),
                dma((pairs,)),
                dma((rows,)),
                dma((rows // 2,)),
                dma((pairs,)),
                dma((pairs,)),
                dma((rows // 2,)),
                dma((2, 2)),
                dma((2,)),
                dma((2,)),
                dma((2,)),
                dma((2, 2)),
                dma((2, 2)),
                dma,
                dma,
            ],
            compiler_params=pltpu.CompilerParams(
                collective_id=0, has_side_effects=True, vmem_limit_bytes=56 * 1024 * 1024
            ),
        )(block_order, columns.reshape(2 * pairs, BLOCK, length))

    placed = (P("col", "row"), P("col"))
    return jax.shard_map(local, mesh=mesh, in_specs=placed, out_specs=P("col", "row"), check_vma=False)
```

```python
import functools

import jax
import jax.numpy as jnp
from jax import lax
from jax.experimental import pallas as pl
from jax.experimental.pallas import tpu as pltpu
from jax.sharding import PartitionSpec as P

BLOCK = 64
PAIR = 2 * BLOCK
STEPS = 4
HALF = BLOCK // 2
PACKED = HALF + 8
UPPER = 1.0 + BLOCK * BLOCK * 0.0905
NN = (((1,), (0,)), ((), ()))
NT = (((1,), (1,)), ((), ()))


def split(a):
    high = a.astype(jnp.bfloat16)
    return high, (a - high.astype(jnp.float32)).astype(jnp.bfloat16)


def split3(a):
    high = a.astype(jnp.bfloat16)
    rest = a - high.astype(jnp.float32)
    middle = rest.astype(jnp.bfloat16)
    return high, middle, (rest - middle.astype(jnp.float32)).astype(jnp.bfloat16)


def product(a, b, dims=NN):
    return lax.dot_general(a, b, dims, preferred_element_type=jnp.float32)


def mm3(a, b):
    (ah, am), (bh, bm) = split(a), split(b)
    count = a.shape[0]
    stacked = product(jnp.concatenate([ah, am], axis=0), bh)
    return stacked[:count] + stacked[count:] + product(ah, bm)


def mm6(a, b, dims=NN):
    (ah, am, al), (bh, bm, bl) = split3(a), split3(b)
    count = a.shape[0]
    first = product(jnp.concatenate([ah, am, al], axis=0), bh, dims)
    second = product(jnp.concatenate([ah, am], axis=0), bm, dims)
    small = first[2 * count :] + second[count:] + product(ah, bl, dims)
    return first[:count] + ((first[count : 2 * count] + second[:count]) + small)


def left(a):
    return a[:, :BLOCK]


def inverse(system, eye):
    low = 2.0 / (1.0 + UPPER)
    y = system * low
    reach = low * (2.0 - low)
    scale = 2.0 / (1.0 + reach)
    x = (scale * low) * (2.0 * eye - y)
    y = scale * (2.0 * y - mm3(left(y), y))
    low = scale * reach
    while low < 0.999:
        reach = low * (2.0 - low)
        scale = 2.0 / (1.0 + reach)
        following = scale * (2.0 * y - mm3(left(y), y))
        x = scale * (2.0 * x - mm3(left(x), y))
        y = following
        low = scale * reach
    return x


def turn_packed(total):
    row = lax.broadcasted_iota(jnp.int32, (HALF, PAIR), 0)
    lane = lax.broadcasted_iota(jnp.int32, (HALF, PAIR), 1)
    cross = total[:HALF]
    norms = total[HALF : HALF + 1]
    bottom_norms = total[HALF + 1 : HALF + 2]
    upper_norms = jnp.sum(jnp.where(lane == row, norms, 0.0), axis=1, keepdims=True)
    lower_norms = jnp.sum(jnp.where(lane == row + HALF, norms, 0.0), axis=1, keepdims=True)
    top_norms = jnp.where(lane < BLOCK, upper_norms, lower_norms)
    spread = bottom_norms - top_norms
    square = spread * spread + 4.0 * cross * cross
    radius = jnp.sqrt(square)
    scale_term = (top_norms + bottom_norms) / BLOCK
    packed = 2.0 * cross * spread / (square + jnp.abs(spread) * radius + scale_term * scale_term)
    rolled = pltpu.roll(packed, BLOCK, 1)
    coupling = jnp.concatenate([jnp.where(lane < BLOCK, packed, rolled), jnp.where(lane < BLOCK, rolled, packed)], axis=0)
    rows = lax.broadcasted_iota(jnp.int32, (BLOCK, PAIR), 0)
    lanes = lax.broadcasted_iota(jnp.int32, (BLOCK, PAIR), 1)
    columns = jnp.where(lanes < BLOCK, lanes, lanes - BLOCK)
    eye = jnp.where(rows == columns, 1.0, 0.0).astype(jnp.float32)
    narrow = left(coupling)
    narrow_t = narrow.T
    system = eye + mm6(narrow, jnp.concatenate([narrow, narrow], axis=0), NT)
    x = inverse(system, eye)
    lower = mm6(narrow_t, x)
    residual = eye - x - mm6(narrow, lower)
    stacked = jnp.concatenate([x, lower], axis=0)
    stacked = stacked + mm3(left(stacked), residual)
    x, lower = stacked[:BLOCK], 2.0 * stacked[BLOCK:]
    corner = eye - mm6(left(lower), coupling)
    diagonal = jnp.sum(jnp.where(rows == columns, corner, 0.0), axis=0, keepdims=True)
    mixed = jnp.where(rows <= columns, 2.0 * x - eye, corner)
    body = jnp.where(lanes < BLOCK, mixed, lower)
    return jnp.concatenate([body, jnp.broadcast_to(diagonal, (8, PAIR))], axis=0)


def unpacked(packed):
    rows = lax.broadcasted_iota(jnp.int32, (BLOCK, PAIR), 0)
    lanes = lax.broadcasted_iota(jnp.int32, (BLOCK, PAIR), 1)
    columns = jnp.where(lanes < BLOCK, lanes, lanes - BLOCK)
    body = packed[:BLOCK]
    flipped = jnp.concatenate([body, body], axis=0).T
    mixed_t, lower_t = flipped[:BLOCK], flipped[BLOCK:]
    moved = pltpu.roll(body, BLOCK, 1)
    top = jnp.where(lanes < BLOCK, jnp.where(rows > columns, mixed_t, body), -lower_t)
    corner = jnp.where(rows == columns, packed[BLOCK : BLOCK + 1], jnp.where(rows > columns, moved, mixed_t))
    bottom = jnp.where(lanes < BLOCK, moved, corner)
    return jnp.concatenate([top, bottom], axis=0)


def gram_packed(block):
    high, low = split(block)
    lefts = jnp.concatenate([high[:BLOCK], low[:BLOCK]], axis=0)
    rights = jnp.concatenate([high[BLOCK:], low[BLOCK:]], axis=0)
    parts = product(lefts, rights, NT)
    halves = parts[:BLOCK] + parts[BLOCK:]
    cross = halves + pltpu.roll(halves, BLOCK, 1)
    lane = lax.broadcasted_iota(jnp.int32, (HALF, PAIR), 1)
    cross = jnp.where(lane < BLOCK, cross[:HALF], cross[HALF:])
    squares = block * block
    partial = squares[:, :128]
    for start in range(128, squares.shape[1], 128):
        partial = partial + squares[:, start : start + 128]
    norms = jnp.broadcast_to(jnp.sum(partial.T, axis=0, keepdims=True), (8, PAIR))
    rows = lax.broadcasted_iota(jnp.int32, (8, PAIR), 0)
    lanes = lax.broadcasted_iota(jnp.int32, (8, PAIR), 1)
    norms = jnp.where(jnp.logical_and(rows == 1, lanes < BLOCK), pltpu.roll(norms, BLOCK, 1), norms)
    return jnp.concatenate([cross, norms], axis=0)


def apply_turn(matrix, block):
    high, low = split(block)
    turn_high, turn_middle, turn_low = split3(matrix)
    lefts = jnp.concatenate([turn_high, turn_middle, turn_low, turn_high], axis=1)
    return product(lefts, jnp.concatenate([high, high, high, low], axis=0))


def turned(packed, block):
    return apply_turn(unpacked(packed), block)


def turned_half(packed, block, side):
    matrix = unpacked(packed)
    return apply_turn(matrix[:BLOCK] if side == 0 else matrix[BLOCK:], block)


def kernel(rows, cols, pairs, order_ref, columns_ref, x1, turns, halos, x0, grams, parts,
           gram_send, gram_recv, turn_send, turn_recv, pass_send, halo_send, halo_recv, relay_send,
           start_send, start_recv, edge_send, edge_recv):
    buffers = (x0, x1)
    me = lax.axis_index("row")
    position = lax.axis_index("col")
    core = lax.rem(me, 2)
    chip = lax.div(me, 2)
    partner = me + 1 - 2 * core
    has_left = position > 0
    has_right = position < cols - 1
    has = (has_left, has_right)
    beside = (position - 1, position + 1)
    last = pairs - 1
    direct = (last % 2, 0)
    half = rows // 2

    barrier = pltpu.get_barrier_semaphore()

    def greet(other, carry):
        @pl.when(other != me)
        def _():
            pl.semaphore_signal(barrier, inc=1, device_id={"row": other})

        for side in (0, 1):
            @pl.when(has[side])
            def _(side=side):
                pl.semaphore_signal(barrier, inc=1, device_id={"row": other, "col": beside[side]})
        return carry

    lax.fori_loop(0, rows, greet, 0)

    def fill(pair):
        for slot in (2 * pair, 2 * pair + 1):
            source = lax.rem(order_ref[slot], 2 * pairs)
            x0[pl.ds(pl.multiple_of(slot * BLOCK + PAIR, BLOCK), BLOCK), :] = columns_ref[source]

    def group_at(place):
        return pairs // 2 - 1 - place, pairs // 2 + place

    fill(0)
    fill(last)
    greeted = rows - 1 + rows * (has_left.astype(jnp.int32) + has_right.astype(jnp.int32))
    pl.semaphore_wait(barrier, greeted)

    def gram_copy(pair):
        return pltpu.make_async_remote_copy(
            src_ref=grams.at[pair], dst_ref=parts.at[me], send_sem=gram_send.at[pair], recv_sem=gram_recv.at[me],
            device_id={"row": pair},
        )

    def gram_arrival(source):
        return pltpu.make_async_remote_copy(
            src_ref=parts.at[source], dst_ref=parts.at[source], send_sem=gram_send.at[0],
            recv_sem=gram_recv.at[source], device_id={"row": partner},
        )

    def turn_copy(other):
        target = jnp.where(other == chip, partner, 2 * other + core)
        return pltpu.make_async_remote_copy(
            src_ref=turns.at[me], dst_ref=turns.at[me], send_sem=turn_send.at[other], recv_sem=turn_recv.at[me],
            device_id={"row": target},
        )

    def pass_copy(pair):
        return pltpu.make_async_remote_copy(
            src_ref=turns.at[pair], dst_ref=turns.at[pair], send_sem=pass_send.at[pair], recv_sem=turn_recv.at[pair],
            device_id={"row": partner},
        )

    def halo_copy(other, side, now):
        return pltpu.make_async_remote_copy(
            src_ref=turns.at[me], dst_ref=halos.at[now, side], send_sem=halo_send.at[other],
            recv_sem=halo_recv.at[now, side], device_id={"row": 2 * other + core, "col": beside[1 - side]},
        )

    def relay_copy(side, now):
        return pltpu.make_async_remote_copy(
            src_ref=halos.at[now, side], dst_ref=halos.at[now, side], send_sem=relay_send.at[side],
            recv_sem=halo_recv.at[now, side], device_id={"row": partner},
        )

    far = (pairs + 1) * PAIR

    def start_copy(side):
        source = pairs * PAIR if side == 0 else PAIR
        target = 0 if side == 0 else far
        return pltpu.make_async_remote_copy(
            src_ref=x0.at[pl.ds(source, PAIR)], dst_ref=x0.at[pl.ds(target, PAIR)], send_sem=start_send.at[side],
            recv_sem=start_recv.at[side], device_id={"col": beside[1 - side]},
        )

    def edge_copy(side, after):
        source = pairs * PAIR if side == 0 else PAIR + BLOCK
        target = 0 if side == 0 else far + BLOCK
        return pltpu.make_async_remote_copy(
            src_ref=buffers[after].at[pl.ds(source, BLOCK)], dst_ref=buffers[after].at[pl.ds(target, BLOCK)],
            send_sem=edge_send.at[after, side], recv_sem=edge_recv.at[after, side],
            device_id={"col": beside[1 - side]},
        )

    for side in (0, 1):
        @pl.when(has[1 - side])
        def _(side=side):
            start_copy(side).start()

    def slot_of(slot, now):
        return buffers[now][pl.ds(pl.multiple_of(slot * PAIR, PAIR), PAIR), :]

    def own():
        def gather(source, carry):
            @pl.when(source != me)
            def _():
                gram_arrival(source).wait_recv()
            return carry

        lax.fori_loop(0, rows, gather, 0)
        total = grams[me]
        for source in range(rows):
            total = total + jnp.where(source == me, 0.0, parts[source])
        turns[me] = turn_packed(total)

    def take_grams(place, now):
        chosen = group_at(place)
        for pair in chosen:
            grams[pair] = gram_packed(slot_of(pair + 1, now))
        for pair in chosen:
            @pl.when(pair != me)
            def _(pair=pair):
                gram_copy(pair).start()

    def first_grams(place, carry):
        for pair in group_at(place):
            fill(pair)
        take_grams(place, 0)
        return carry

    lax.fori_loop(0, pairs // 2 - 1, first_grams, 0)
    take_grams(pairs // 2 - 1, 0)

    def step(index):
        now, after = index % 2, 1 - index % 2
        later = buffers[after]
        ending = index == STEPS - 1

        @pl.when(me < pairs)
        def _():
            own()

            def spread_out(other, carry):
                turn_copy(other).start()
                return carry

            lax.fori_loop(0, half, spread_out, 0)

        for side, owner in ((0, last), (1, 0)):
            @pl.when(jnp.logical_and(me == owner, has[1 - side]))
            def _(side=side):
                def spread_halo(other, carry):
                    halo_copy(other, side, now).start()
                    return carry

                lax.fori_loop(0, half, spread_halo, 0)

        def settle_gram(pair, carry):
            @pl.when(pair != me)
            def _():
                gram_copy(pair).wait_send()
            return carry

        lax.fori_loop(0, pairs, settle_gram, 0)

        for side in (0, 1):
            @pl.when(has[1 - side])
            def _(side=side):
                if index > 1:
                    edge_copy(side, after).wait_send()
                if index == 1:
                    start_copy(side).wait_send()

        def relay(pair):
            @pl.when(jnp.logical_and(pair != me, lax.rem(pair, 2) == core))
            def _():
                pass_copy(pair).wait_recv()
                pass_copy(pair).start()

        def relay_group(place):
            for pair in group_at(place):
                relay(pair)

        def receive_group(place):
            for pair in group_at(place):
                @pl.when(jnp.logical_and(pair != me, lax.rem(pair, 2) != core))
                def _(pair=pair):
                    pass_copy(pair).wait_recv()

        def settle_group(place):
            for pair in group_at(place):
                @pl.when(jnp.logical_and(pair != me, lax.rem(pair, 2) == core))
                def _(pair=pair):
                    pass_copy(pair).wait_send()

        def apply_group(place):
            chosen = group_at(place)
            results = [turned(turns[pair], slot_of(pair + 1, now)) for pair in chosen]
            for pair, result in zip(chosen, results):
                opening = jnp.logical_and(pair == 0, jnp.logical_not(has_left))
                closing = jnp.logical_and(pair == last, jnp.logical_not(has_right))
                top = jnp.where(opening, PAIR, jnp.where(closing, pairs * PAIR + BLOCK, (pair + 2) * PAIR))
                bottom = jnp.where(opening, 2 * PAIR, pair * PAIR + BLOCK)
                later[pl.ds(pl.multiple_of(top, BLOCK), BLOCK), :] = result[:BLOCK]
                later[pl.ds(pl.multiple_of(bottom, BLOCK), BLOCK), :] = result[BLOCK:]

        def next_grams(place):
            settle_group(place)
            take_grams(place, after)

        if ending:
            for place in range(pairs // 2):
                relay_group(place)
            for place in range(pairs // 2):
                receive_group(place)
        else:
            for place in range(2):
                relay_group(place)
            receive_group(0)
            apply_group(0)

        def apply_next(place, carry):
            @pl.when(place < pairs // 2 - 1)
            def _():
                relay_group(place + 1)

            receive_group(place)
            apply_group(place)
            next_grams(place - 1)
            return carry

        if not ending:
            lax.fori_loop(1, pairs // 2, apply_next, 0)

        def receive_halo(side):
            @pl.when(has[side])
            def _():
                relay_copy(side, now).wait_recv()

                @pl.when(core == direct[side])
                def _():
                    relay_copy(side, now).start()

        for relayed in (False, True):
            for side in (0, 1):
                @pl.when((core != direct[side]) == relayed)
                def _(side=side):
                    receive_halo(side)

        for side in (0, 1):
            @pl.when(has[side])
            def _(side=side):
                if index == 0:
                    start_copy(side).wait_recv()
                else:
                    edge_copy(side, now).wait_recv()
                if not ending:
                    rest = turned_half(halos[now, side], slot_of(side * (pairs + 1), now), side)
                    target = PAIR if side == 0 else pairs * PAIR + BLOCK
                    later[pl.ds(target, BLOCK), :] = rest

        if ending:
            for place in range(pairs // 2):
                settle_group(place)
        else:
            next_grams(pairs // 2 - 1)
        for side in (0, 1):
            @pl.when(jnp.logical_and(core == direct[side], has[side]))
            def _(side=side):
                relay_copy(side, now).wait_send()

        if not ending:
            for side in (0, 1):
                @pl.when(has[1 - side])
                def _(side=side):
                    edge_copy(side, after).start()

        @pl.when(me < pairs)
        def _():
            def settle_turn(other, carry):
                turn_copy(other).wait_send()
                return carry

            lax.fori_loop(0, half, settle_turn, 0)

        for side, owner in ((0, last), (1, 0)):
            @pl.when(jnp.logical_and(me == owner, has[1 - side]))
            def _(side=side):
                def settle_halo(other, carry):
                    halo_copy(other, side, now).wait_send()
                    return carry

                lax.fori_loop(0, half, settle_halo, 0)

    for index in range(STEPS):
        step(index)
    for side in (0, 1):
        @pl.when(has[1 - side])
        def _(side=side):
            edge_copy(side, (STEPS - 1) % 2).wait_send()


def closing_kernel(cols, pairs, x, turns, halos, out_ref, result, out_sem):
    position = lax.axis_index("col")
    has = (position > 0, position < cols - 1)
    last = pairs - 1
    now = (STEPS - 1) % 2

    def out_copy(place, row):
        rows = pl.ds(pl.multiple_of(row, BLOCK), BLOCK)
        return pltpu.make_async_copy(result.at[rows], out_ref.at[rows], out_sem.at[place])

    def slot_of(slot):
        return x[pl.ds(pl.multiple_of(slot * PAIR, PAIR), PAIR), :]

    def put(row, values):
        result[pl.ds(pl.multiple_of(row, BLOCK), BLOCK), :] = values

    def inner(place, carry):
        chosen = (2 * place + 1, 2 * place + 2)
        results = [turned(turns[pair], slot_of(pair + 1)) for pair in chosen]
        for pair, both in zip(chosen, results):
            for part, row in enumerate(((pair + 1) * PAIR, (pair - 1) * PAIR + BLOCK)):
                put(row, both[part * BLOCK : (part + 1) * BLOCK])
        for pair in chosen:
            for part, row in enumerate(((pair + 1) * PAIR, (pair - 1) * PAIR + BLOCK)):
                out_copy(2 * pair + part, row).start()
        return carry

    lax.fori_loop(0, (pairs - 2) // 2, inner, 0)
    results = [turned(turns[pair], slot_of(pair + 1)) for pair in (0, last)]
    first_top = jnp.where(has[0], PAIR, 0)
    put(first_top, results[0][:BLOCK])
    put((last - 1) * PAIR + BLOCK, results[1][BLOCK:])
    kept = (jnp.where(has[0], pairs * PAIR, PAIR), jnp.where(has[1], pairs * PAIR + BLOCK, last * PAIR + BLOCK))
    put(kept[0], results[0][BLOCK:])
    put(kept[1], results[1][:BLOCK])
    out_copy(0, first_top).start()
    out_copy(1, (last - 1) * PAIR + BLOCK).start()
    for side in (0, 1):
        @pl.when(jnp.logical_not(has[side]))
        def _(side=side):
            out_copy(2 * last + side, kept[side]).start()

        @pl.when(has[side])
        def _(side=side):
            target = 0 if side == 0 else last * PAIR + BLOCK
            put(target, turned_half(halos[now, side], slot_of(side * (pairs + 1)), side))
            out_copy(2 * last + side, target).start()

    def settle(place, carry):
        out_copy(place, 0).wait()
        return carry

    lax.fori_loop(0, 2 * pairs, settle, 0)


def solution(mesh):
    rows, cols = mesh.shape["row"], mesh.shape["col"]

    def local(columns, block_order):
        width, length = columns.shape
        pairs = width // PAIR
        assert 4 <= pairs <= rows and rows % pairs == 0 and pairs & (pairs - 1) == 0 and STEPS % 2 == 0
        dma = pltpu.SemaphoreType.DMA
        wide = (width + 2 * PAIR, length)
        vmem = pl.BlockSpec(memory_space=pltpu.VMEM)
        state = pl.pallas_call(
            functools.partial(kernel, rows, cols, pairs),
            out_shape=[
                jax.ShapeDtypeStruct(wide, jnp.float32),
                jax.ShapeDtypeStruct((pairs, BLOCK + 8, PAIR), jnp.float32),
                jax.ShapeDtypeStruct((2, 2, BLOCK + 8, PAIR), jnp.float32),
            ],
            in_specs=[pl.BlockSpec(memory_space=pltpu.SMEM), vmem],
            out_specs=[vmem, vmem, vmem],
            scratch_shapes=[
                pltpu.VMEM(wide, jnp.float32),
                pltpu.VMEM((pairs, PACKED, PAIR), jnp.float32),
                pltpu.VMEM((rows, PACKED, PAIR), jnp.float32),
                dma((pairs,)),
                dma((rows,)),
                dma((rows // 2,)),
                dma((pairs,)),
                dma((pairs,)),
                dma((rows // 2,)),
                dma((2, 2)),
                dma((2,)),
                dma((2,)),
                dma((2,)),
                dma((2, 2)),
                dma((2, 2)),
            ],
            compiler_params=pltpu.CompilerParams(
                collective_id=0, has_side_effects=True, vmem_limit_bytes=20 * 1024 * 1024
            ),
        )(block_order, columns.reshape(2 * pairs, BLOCK, length))
        return pl.pallas_call(
            functools.partial(closing_kernel, cols, pairs),
            out_shape=jax.ShapeDtypeStruct((width, length), jnp.float32),
            in_specs=[vmem, vmem, vmem],
            out_specs=pl.BlockSpec(memory_space=pl.ANY),
            scratch_shapes=[pltpu.VMEM((width + PAIR, length), jnp.float32), dma((2 * pairs,))],
            compiler_params=pltpu.CompilerParams(vmem_limit_bytes=20 * 1024 * 1024),
        )(*state)

    placed = (P("col", "row"), P("col"))
    return jax.shard_map(local, mesh=mesh, in_specs=placed, out_specs=P("col", "row"), check_vma=False)
```

```python
import functools

import jax
import jax.numpy as jnp
from jax import lax
from jax.experimental import pallas as pl
from jax.experimental.pallas import tpu as pltpu
from jax.sharding import PartitionSpec as P

BLOCK = 64
PAIR = 2 * BLOCK
STEPS = 4
HALF = BLOCK // 2
PACKED = HALF + 8
UPPER = 1.0 + BLOCK * BLOCK * 0.0905
NN = (((1,), (0,)), ((), ()))
NT = (((1,), (1,)), ((), ()))


def split(a):
    high = a.astype(jnp.bfloat16)
    return high, (a - high.astype(jnp.float32)).astype(jnp.bfloat16)


def split3(a):
    high = a.astype(jnp.bfloat16)
    rest = a - high.astype(jnp.float32)
    middle = rest.astype(jnp.bfloat16)
    return high, middle, (rest - middle.astype(jnp.float32)).astype(jnp.bfloat16)


def product(a, b, dims=NN):
    return lax.dot_general(a, b, dims, preferred_element_type=jnp.float32)


def mm3(a, b, dims=NN):
    (ah, am), (bh, bm) = split(a), split(b)
    count = a.shape[0]
    stacked = product(jnp.concatenate([ah, am], axis=0), bh, dims)
    return stacked[:count] + stacked[count:] + product(ah, bm, dims)


def mm6(a, b, dims=NN):
    (ah, am, al), (bh, bm, bl) = split3(a), split3(b)
    count = a.shape[0]
    first = product(jnp.concatenate([ah, am, al], axis=0), bh, dims)
    second = product(jnp.concatenate([ah, am], axis=0), bm, dims)
    small = first[2 * count :] + second[count:] + product(ah, bl, dims)
    return first[:count] + ((first[count : 2 * count] + second[:count]) + small)


def left(a):
    return a[:, :BLOCK]


def inverse(system, eye):
    low = 2.0 / (1.0 + UPPER)
    y = system * low
    reach = low * (2.0 - low)
    scale = 2.0 / (1.0 + reach)
    x = (scale * low) * (2.0 * eye - y)
    y = scale * (2.0 * y - mm3(left(y), y))
    low = scale * reach
    while low < 0.999:
        reach = low * (2.0 - low)
        scale = 2.0 / (1.0 + reach)
        following = scale * (2.0 * y - mm3(left(y), y))
        x = scale * (2.0 * x - mm3(left(x), y))
        y = following
        low = scale * reach
    return x


def coupling_packed(total):
    row = lax.broadcasted_iota(jnp.int32, (HALF, PAIR), 0)
    lane = lax.broadcasted_iota(jnp.int32, (HALF, PAIR), 1)
    cross = total[:HALF]
    norms = total[HALF : HALF + 1]
    bottom_norms = total[HALF + 1 : HALF + 2]
    upper_norms = jnp.sum(jnp.where(lane == row, norms, 0.0), axis=1, keepdims=True)
    lower_norms = jnp.sum(jnp.where(lane == row + HALF, norms, 0.0), axis=1, keepdims=True)
    top_norms = jnp.where(lane < BLOCK, upper_norms, lower_norms)
    spread = bottom_norms - top_norms
    square = spread * spread + 4.0 * cross * cross
    radius = jnp.sqrt(square)
    scale_term = (top_norms + bottom_norms) / BLOCK
    return 2.0 * cross * spread / (square + jnp.abs(spread) * radius + scale_term * scale_term)


def doubled(packed):
    lane = lax.broadcasted_iota(jnp.int32, (HALF, PAIR), 1)
    rolled = pltpu.roll(packed, BLOCK, 1)
    return jnp.concatenate([jnp.where(lane < BLOCK, packed, rolled), jnp.where(lane < BLOCK, rolled, packed)], axis=0)


def inverse_packed(packed):
    coupling = doubled(packed)
    rows = lax.broadcasted_iota(jnp.int32, (BLOCK, PAIR), 0)
    lanes = lax.broadcasted_iota(jnp.int32, (BLOCK, PAIR), 1)
    columns = jnp.where(lanes < BLOCK, lanes, lanes - BLOCK)
    eye = jnp.where(rows == columns, 1.0, 0.0).astype(jnp.float32)
    narrow = left(coupling)
    narrow_t = narrow.T
    system = eye + mm3(narrow, jnp.concatenate([narrow, narrow], axis=0), NT)
    x = inverse(system, eye)
    residual = eye - x - mm6(narrow, mm6(narrow_t, x))
    x = x + mm3(left(x), residual)
    return jnp.where(lanes[:HALF] < BLOCK, x[:HALF], x[HALF:])


def lefts_of(matrix):
    lane = lax.broadcasted_iota(jnp.int32, (BLOCK, PAIR), 1)
    high = matrix.astype(jnp.bfloat16).astype(jnp.float32)
    rest = matrix - high
    middle = rest.astype(jnp.bfloat16).astype(jnp.float32)
    first = jnp.where(lane < BLOCK, high, middle)
    second = jnp.where(lane < BLOCK, rest - middle, high)
    return jnp.concatenate([first, second], axis=1).astype(jnp.bfloat16)


def rights_of(block):
    high, low = split(block)
    return jnp.concatenate([high, high, high, low], axis=0)


def opened(packed, block):
    coupling = doubled(packed)
    flipped = jnp.concatenate([coupling, coupling], axis=0).T[:BLOCK]
    return block[:BLOCK] - product(lefts_of(coupling), rights_of(block[BLOCK:])), lefts_of(flipped)


def upper_solved(packed, rest):
    return product(lefts_of(doubled(packed)), rights_of(rest))


def lower_solved(flip, upper, block):
    return block[BLOCK:] + product(flip, rights_of(upper))


def turned(packed, rest, flip, block):
    upper = upper_solved(packed, rest)
    return 2.0 * upper - block[:BLOCK], 2.0 * lower_solved(flip, upper, block) - block[BLOCK:]


def turned_half(packed, rest, flip, block, side):
    upper = upper_solved(packed, rest)
    if side == 0:
        return 2.0 * upper - block[:BLOCK]
    return 2.0 * lower_solved(flip, upper, block) - block[BLOCK:]


def gram_packed(block):
    high, low = split(block)
    lefts = jnp.concatenate([high[:BLOCK], low[:BLOCK]], axis=0)
    rights = jnp.concatenate([high[BLOCK:], low[BLOCK:]], axis=0)
    parts = product(lefts, rights, NT)
    halves = parts[:BLOCK] + parts[BLOCK:]
    cross = halves + pltpu.roll(halves, BLOCK, 1)
    lane = lax.broadcasted_iota(jnp.int32, (HALF, PAIR), 1)
    cross = jnp.where(lane < BLOCK, cross[:HALF], cross[HALF:])
    squares = block * block
    partial = squares[:, :128]
    for start in range(128, squares.shape[1], 128):
        partial = partial + squares[:, start : start + 128]
    norms = jnp.broadcast_to(jnp.sum(partial.T, axis=0, keepdims=True), (8, PAIR))
    rows = lax.broadcasted_iota(jnp.int32, (8, PAIR), 0)
    lanes = lax.broadcasted_iota(jnp.int32, (8, PAIR), 1)
    norms = jnp.where(jnp.logical_and(rows == 1, lanes < BLOCK), pltpu.roll(norms, BLOCK, 1), norms)
    return jnp.concatenate([cross, norms], axis=0)


def kernel(rows, cols, pairs, order_ref, columns_ref, x1, couplings, inverses, halo_couplings, halo_inverses,
           x0, grams, parts, rests, flips, gram_send, gram_recv, coupling_send, coupling_recv, inverse_send,
           inverse_recv, halo_send, halo_recv, start_send, start_recv, edge_send, edge_recv):
    buffers = (x0, x1)
    me = lax.axis_index("row")
    position = lax.axis_index("col")
    partner = jnp.bitwise_xor(me, 1)
    has_left = position > 0
    has_right = position < cols - 1
    has = (has_left, has_right)
    beside = (position - 1, position + 1)
    last = pairs - 1
    kinds = ((couplings, halo_couplings, coupling_send, coupling_recv), (inverses, halo_inverses, inverse_send, inverse_recv))

    barrier = pltpu.get_barrier_semaphore()

    def greet(other, carry):
        @pl.when(other != me)
        def _():
            pl.semaphore_signal(barrier, inc=1, device_id={"row": other})

        for side in (0, 1):
            @pl.when(has[side])
            def _(side=side):
                pl.semaphore_signal(barrier, inc=1, device_id={"row": other, "col": beside[side]})
        return carry

    lax.fori_loop(0, rows, greet, 0)

    def fill(pair):
        for slot in (2 * pair, 2 * pair + 1):
            source = lax.rem(order_ref[slot], 2 * pairs)
            x0[pl.ds(pl.multiple_of(slot * BLOCK + PAIR, BLOCK), BLOCK), :] = columns_ref[source]

    def group_at(place):
        return pairs // 2 - 1 - place, pairs // 2 + place

    fill(0)
    fill(last)
    greeted = rows - 1 + rows * (has_left.astype(jnp.int32) + has_right.astype(jnp.int32))
    pl.semaphore_wait(barrier, greeted)

    def gram_copy(pair):
        return pltpu.make_async_remote_copy(
            src_ref=grams.at[pair], dst_ref=parts.at[me], send_sem=gram_send.at[pair], recv_sem=gram_recv.at[me],
            device_id={"row": pair},
        )

    def gram_arrival(source):
        return pltpu.make_async_remote_copy(
            src_ref=parts.at[source], dst_ref=parts.at[source], send_sem=gram_send.at[0],
            recv_sem=gram_recv.at[source], device_id={"row": partner},
        )

    def spread_copy(kind, other):
        values, _, send, recv = kinds[kind]
        return pltpu.make_async_remote_copy(
            src_ref=values.at[me], dst_ref=values.at[me], send_sem=send.at[other], recv_sem=recv.at[me],
            device_id={"row": jnp.bitwise_xor(me, other)},
        )

    def spread_arrival(kind, pair):
        values, _, send, recv = kinds[kind]
        return pltpu.make_async_remote_copy(
            src_ref=values.at[pair], dst_ref=values.at[pair], send_sem=send.at[0], recv_sem=recv.at[pair],
            device_id={"row": partner},
        )

    def halo_copy(kind, other, side, now):
        values, halo, _, _ = kinds[kind]
        return pltpu.make_async_remote_copy(
            src_ref=values.at[me], dst_ref=halo.at[now, side], send_sem=halo_send.at[kind, other],
            recv_sem=halo_recv.at[kind, now, side],
            device_id={"row": jnp.bitwise_xor(me, other), "col": beside[1 - side]},
        )

    def halo_arrival(kind, side, now):
        halo = kinds[kind][1]
        return pltpu.make_async_remote_copy(
            src_ref=halo.at[now, side], dst_ref=halo.at[now, side], send_sem=halo_send.at[kind, 0],
            recv_sem=halo_recv.at[kind, now, side], device_id={"row": partner},
        )

    far = (pairs + 1) * PAIR

    def start_copy(side):
        source = pairs * PAIR if side == 0 else PAIR
        target = 0 if side == 0 else far
        return pltpu.make_async_remote_copy(
            src_ref=x0.at[pl.ds(source, PAIR)], dst_ref=x0.at[pl.ds(target, PAIR)], send_sem=start_send.at[side],
            recv_sem=start_recv.at[side], device_id={"col": beside[1 - side]},
        )

    def edge_copy(side, after):
        source = pairs * PAIR if side == 0 else PAIR + BLOCK
        target = 0 if side == 0 else far + BLOCK
        return pltpu.make_async_remote_copy(
            src_ref=buffers[after].at[pl.ds(source, BLOCK)], dst_ref=buffers[after].at[pl.ds(target, BLOCK)],
            send_sem=edge_send.at[after, side], recv_sem=edge_recv.at[after, side],
            device_id={"col": beside[1 - side]},
        )

    for side in (0, 1):
        @pl.when(has[1 - side])
        def _(side=side):
            start_copy(side).start()

    def slot_of(slot, now):
        return buffers[now][pl.ds(pl.multiple_of(slot * PAIR, PAIR), PAIR), :]

    def spread(kind, now):
        def spread_out(place, carry):
            spread_copy(kind, rows - place).start()
            return carry

        lax.fori_loop(1, rows, spread_out, 0)
        for side, owner in ((0, last), (1, 0)):
            @pl.when(jnp.logical_and(me == owner, has[1 - side]))
            def _(side=side):
                def spread_halo(place, carry):
                    halo_copy(kind, rows - place, side, now).start()
                    return carry

                lax.fori_loop(1, rows + 1, spread_halo, 0)

    def settle_spread(kind, now):
        def settle_out(other, carry):
            spread_copy(kind, other).wait_send()
            return carry

        lax.fori_loop(1, rows, settle_out, 0)
        for side, owner in ((0, last), (1, 0)):
            @pl.when(jnp.logical_and(me == owner, has[1 - side]))
            def _(side=side):
                def settle_halo(other, carry):
                    halo_copy(kind, other, side, now).wait_send()
                    return carry

                lax.fori_loop(0, rows, settle_halo, 0)

    def own(now):
        def gather(source, carry):
            @pl.when(source != me)
            def _():
                gram_arrival(source).wait_recv()
            return carry

        lax.fori_loop(0, rows, gather, 0)
        total = grams[me]
        for source in range(rows):
            total = total + jnp.where(source == me, 0.0, parts[source])
        couplings[me] = coupling_packed(total)
        spread(0, now)
        inverses[me] = inverse_packed(couplings[me])
        spread(1, now)

    def take_grams(place, now):
        chosen = group_at(place)
        for pair in chosen:
            grams[pair] = gram_packed(slot_of(pair + 1, now))
        for pair in chosen:
            @pl.when(pair != me)
            def _(pair=pair):
                gram_copy(pair).start()

    def first_grams(place, carry):
        for pair in group_at(place):
            fill(pair)
        take_grams(place, 0)
        return carry

    lax.fori_loop(0, pairs // 2 - 1, first_grams, 0)
    take_grams(pairs // 2 - 1, 0)

    def step(index):
        now, after = index % 2, 1 - index % 2
        later = buffers[after]
        ending = index == STEPS - 1

        @pl.when(me < pairs)
        def _():
            own(now)

        def settle_gram(pair, carry):
            @pl.when(pair != me)
            def _():
                gram_copy(pair).wait_send()
            return carry

        lax.fori_loop(0, pairs, settle_gram, 0)

        for side in (0, 1):
            @pl.when(has[1 - side])
            def _(side=side):
                if index > 1:
                    edge_copy(side, after).wait_send()
                if index == 1:
                    start_copy(side).wait_send()

        def receive(kind, place):
            for pair in group_at(place):
                @pl.when(pair != me)
                def _(pair=pair):
                    spread_arrival(kind, pair).wait_recv()

        def receive_halo(kind, side):
            halo_arrival(kind, side, now).wait_recv()
            if kind == 0:
                if index == 0:
                    start_copy(side).wait_recv()
                else:
                    edge_copy(side, now).wait_recv()

        def open_group(place):
            receive(0, place)
            for pair in group_at(place):
                rests[pair + 1], flips[pair + 1] = opened(couplings[pair], slot_of(pair + 1, now))

        def close_group(place):
            receive(1, place)
            chosen = group_at(place)
            results = [turned(inverses[pair], rests[pair + 1], flips[pair + 1], slot_of(pair + 1, now)) for pair in chosen]
            for pair, (upper, lower) in zip(chosen, results):
                opening = jnp.logical_and(pair == 0, jnp.logical_not(has_left))
                closing = jnp.logical_and(pair == last, jnp.logical_not(has_right))
                top = jnp.where(opening, PAIR, jnp.where(closing, pairs * PAIR + BLOCK, (pair + 2) * PAIR))
                bottom = jnp.where(opening, 2 * PAIR, pair * PAIR + BLOCK)
                later[pl.ds(pl.multiple_of(top, BLOCK), BLOCK), :] = upper
                later[pl.ds(pl.multiple_of(bottom, BLOCK), BLOCK), :] = lower

        if ending:
            for kind in (0, 1):
                for place in range(pairs // 2):
                    receive(kind, place)
                for side in (0, 1):
                    @pl.when(has[side])
                    def _(kind=kind, side=side):
                        receive_halo(kind, side)
        else:
            open_group(0)
            open_group(1)
            close_group(0)

            def close_next(place, carry):
                @pl.when(place < pairs // 2 - 1)
                def _():
                    open_group(place + 1)

                close_group(place)
                take_grams(place - 1, after)
                return carry

            lax.fori_loop(1, pairs // 2, close_next, 0)
            for side in (0, 1):
                @pl.when(has[side])
                def _(side=side):
                    slot = side * (pairs + 1)
                    receive_halo(0, side)
                    rests[slot], flips[slot] = opened(halo_couplings[now, side], slot_of(slot, now))

            for side in (0, 1):
                @pl.when(has[side])
                def _(side=side):
                    slot = side * (pairs + 1)
                    receive_halo(1, side)
                    target = PAIR if side == 0 else pairs * PAIR + BLOCK
                    later[pl.ds(target, BLOCK), :] = turned_half(
                        halo_inverses[now, side], rests[slot], flips[slot], slot_of(slot, now), side
                    )

            take_grams(pairs // 2 - 1, after)
            for side in (0, 1):
                @pl.when(has[1 - side])
                def _(side=side):
                    edge_copy(side, after).start()

        @pl.when(me < pairs)
        def _():
            for kind in (0, 1):
                settle_spread(kind, now)

    for index in range(STEPS):
        step(index)
    for side in (0, 1):
        @pl.when(has[1 - side])
        def _(side=side):
            edge_copy(side, (STEPS - 1) % 2).wait_send()


def closing_kernel(cols, pairs, x, couplings, inverses, halo_couplings, halo_inverses, out_ref, result, out_sem):
    position = lax.axis_index("col")
    has = (position > 0, position < cols - 1)
    last = pairs - 1
    now = (STEPS - 1) % 2

    def out_copy(place, row):
        rows = pl.ds(pl.multiple_of(row, BLOCK), BLOCK)
        return pltpu.make_async_copy(result.at[rows], out_ref.at[rows], out_sem.at[place])

    def slot_of(slot):
        return x[pl.ds(pl.multiple_of(slot * PAIR, PAIR), PAIR), :]

    def put(row, values):
        result[pl.ds(pl.multiple_of(row, BLOCK), BLOCK), :] = values

    def finished(pair):
        block = slot_of(pair + 1)
        return turned(inverses[pair], *opened(couplings[pair], block), block)

    def finished_half(side):
        block = slot_of(side * (pairs + 1))
        return turned_half(halo_inverses[now, side], *opened(halo_couplings[now, side], block), block, side)

    def inner(place, carry):
        chosen = (2 * place + 1, 2 * place + 2)
        results = [finished(pair) for pair in chosen]
        for pair, both in zip(chosen, results):
            for part, row in enumerate(((pair + 1) * PAIR, (pair - 1) * PAIR + BLOCK)):
                put(row, both[part])
        for pair in chosen:
            for part, row in enumerate(((pair + 1) * PAIR, (pair - 1) * PAIR + BLOCK)):
                out_copy(2 * pair + part, row).start()
        return carry

    lax.fori_loop(0, (pairs - 2) // 2, inner, 0)
    results = [finished(pair) for pair in (0, last)]
    first_top = jnp.where(has[0], PAIR, 0)
    put(first_top, results[0][0])
    put((last - 1) * PAIR + BLOCK, results[1][1])
    kept = (jnp.where(has[0], pairs * PAIR, PAIR), jnp.where(has[1], pairs * PAIR + BLOCK, last * PAIR + BLOCK))
    put(kept[0], results[0][1])
    put(kept[1], results[1][0])
    out_copy(0, first_top).start()
    out_copy(1, (last - 1) * PAIR + BLOCK).start()
    for side in (0, 1):
        @pl.when(jnp.logical_not(has[side]))
        def _(side=side):
            out_copy(2 * last + side, kept[side]).start()

        @pl.when(has[side])
        def _(side=side):
            target = 0 if side == 0 else last * PAIR + BLOCK
            put(target, finished_half(side))
            out_copy(2 * last + side, target).start()

    def settle(place, carry):
        out_copy(place, 0).wait()
        return carry

    lax.fori_loop(0, 2 * pairs, settle, 0)


def solution(mesh):
    rows, cols = mesh.shape["row"], mesh.shape["col"]

    def local(columns, block_order):
        width, length = columns.shape
        pairs = width // PAIR
        assert 4 <= pairs <= rows and rows % pairs == 0 and rows & (rows - 1) == 0 and STEPS % 2 == 0
        dma = pltpu.SemaphoreType.DMA
        wide = (width + 2 * PAIR, length)
        vmem = pl.BlockSpec(memory_space=pltpu.VMEM)
        state = pl.pallas_call(
            functools.partial(kernel, rows, cols, pairs),
            out_shape=[
                jax.ShapeDtypeStruct(wide, jnp.float32),
                jax.ShapeDtypeStruct((pairs, HALF, PAIR), jnp.float32),
                jax.ShapeDtypeStruct((pairs, HALF, PAIR), jnp.float32),
                jax.ShapeDtypeStruct((2, 2, HALF, PAIR), jnp.float32),
                jax.ShapeDtypeStruct((2, 2, HALF, PAIR), jnp.float32),
            ],
            in_specs=[pl.BlockSpec(memory_space=pltpu.SMEM), vmem],
            out_specs=[vmem] * 5,
            scratch_shapes=[
                pltpu.VMEM(wide, jnp.float32),
                pltpu.VMEM((pairs, PACKED, PAIR), jnp.float32),
                pltpu.VMEM((rows, PACKED, PAIR), jnp.float32),
                pltpu.VMEM((pairs + 2, BLOCK, length), jnp.float32),
                pltpu.VMEM((pairs + 2, BLOCK, 2 * PAIR), jnp.bfloat16),
                dma((pairs,)),
                dma((rows,)),
                dma((rows,)),
                dma((pairs,)),
                dma((rows,)),
                dma((pairs,)),
                dma((2, rows)),
                dma((2, 2, 2)),
                dma((2,)),
                dma((2,)),
                dma((2, 2)),
                dma((2, 2)),
            ],
            compiler_params=pltpu.CompilerParams(
                collective_id=0, has_side_effects=True, vmem_limit_bytes=20 * 1024 * 1024
            ),
        )(block_order, columns.reshape(2 * pairs, BLOCK, length))
        return pl.pallas_call(
            functools.partial(closing_kernel, cols, pairs),
            out_shape=jax.ShapeDtypeStruct((width, length), jnp.float32),
            in_specs=[vmem] * 5,
            out_specs=pl.BlockSpec(memory_space=pl.ANY),
            scratch_shapes=[pltpu.VMEM((width + PAIR, length), jnp.float32), dma((2 * pairs,))],
            compiler_params=pltpu.CompilerParams(vmem_limit_bytes=20 * 1024 * 1024),
        )(*state)

    placed = (P("col", "row"), P("col"))
    return jax.shard_map(local, mesh=mesh, in_specs=placed, out_specs=P("col", "row"), check_vma=False)
```

```python
import functools

import jax
import jax.numpy as jnp
from jax import lax
from jax.experimental import pallas as pl
from jax.experimental.pallas import tpu as pltpu
from jax.sharding import PartitionSpec as P

BLOCK = 64
PAIR = 2 * BLOCK
STEPS = 4
HALF = BLOCK // 2
PACKED = HALF + 8
UPPER = 1.0 + BLOCK * BLOCK * 0.0905
NN = (((1,), (0,)), ((), ()))
NT = (((1,), (1,)), ((), ()))


def split(a):
    high = a.astype(jnp.bfloat16)
    return high, (a - high.astype(jnp.float32)).astype(jnp.bfloat16)


def split3(a):
    high = a.astype(jnp.bfloat16)
    rest = a - high.astype(jnp.float32)
    middle = rest.astype(jnp.bfloat16)
    return high, middle, (rest - middle.astype(jnp.float32)).astype(jnp.bfloat16)


def product(a, b, dims=NN):
    return lax.dot_general(a, b, dims, preferred_element_type=jnp.float32)


def mm3(a, b, dims=NN):
    (ah, am), (bh, bm) = split(a), split(b)
    count = a.shape[0]
    stacked = product(jnp.concatenate([ah, am], axis=0), bh, dims)
    return stacked[:count] + stacked[count:] + product(ah, bm, dims)


def mm6(a, b, dims=NN):
    (ah, am, al), (bh, bm, bl) = split3(a), split3(b)
    count = a.shape[0]
    first = product(jnp.concatenate([ah, am, al], axis=0), bh, dims)
    second = product(jnp.concatenate([ah, am], axis=0), bm, dims)
    small = first[2 * count :] + second[count:] + product(ah, bl, dims)
    return first[:count] + ((first[count : 2 * count] + second[:count]) + small)


def left(a):
    return a[:, :BLOCK]


def inverse(system, eye):
    low = 2.0 / (1.0 + UPPER)
    y = system * low
    reach = low * (2.0 - low)
    scale = 2.0 / (1.0 + reach)
    x = (scale * low) * (2.0 * eye - y)
    y = scale * (2.0 * y - mm3(left(y), y))
    low = scale * reach
    while low < 0.999:
        reach = low * (2.0 - low)
        scale = 2.0 / (1.0 + reach)
        following = scale * (2.0 * y - mm3(left(y), y))
        x = scale * (2.0 * x - mm3(left(x), y))
        y = following
        low = scale * reach
    return x


def coupling_packed(total):
    row = lax.broadcasted_iota(jnp.int32, (HALF, PAIR), 0)
    lane = lax.broadcasted_iota(jnp.int32, (HALF, PAIR), 1)
    cross = total[:HALF]
    norms = total[HALF : HALF + 1]
    bottom_norms = total[HALF + 1 : HALF + 2]
    upper_norms = jnp.sum(jnp.where(lane == row, norms, 0.0), axis=1, keepdims=True)
    lower_norms = jnp.sum(jnp.where(lane == row + HALF, norms, 0.0), axis=1, keepdims=True)
    top_norms = jnp.where(lane < BLOCK, upper_norms, lower_norms)
    spread = bottom_norms - top_norms
    square = spread * spread + 4.0 * cross * cross
    radius = jnp.sqrt(square)
    scale_term = (top_norms + bottom_norms) / BLOCK
    return 2.0 * cross * spread / (square + jnp.abs(spread) * radius + scale_term * scale_term)


def doubled(packed):
    lane = lax.broadcasted_iota(jnp.int32, (HALF, PAIR), 1)
    rolled = pltpu.roll(packed, BLOCK, 1)
    return jnp.concatenate([jnp.where(lane < BLOCK, packed, rolled), jnp.where(lane < BLOCK, rolled, packed)], axis=0)


def inverse_packed(packed):
    coupling = doubled(packed)
    rows = lax.broadcasted_iota(jnp.int32, (BLOCK, PAIR), 0)
    lanes = lax.broadcasted_iota(jnp.int32, (BLOCK, PAIR), 1)
    columns = jnp.where(lanes < BLOCK, lanes, lanes - BLOCK)
    eye = jnp.where(rows == columns, 1.0, 0.0).astype(jnp.float32)
    narrow = left(coupling)
    narrow_t = narrow.T
    system = eye + mm3(narrow, jnp.concatenate([narrow, narrow], axis=0), NT)
    x = inverse(system, eye)
    residual = eye - x - mm6(narrow, mm6(narrow_t, x))
    x = x + mm3(left(x), residual)
    return jnp.where(lanes[:HALF] < BLOCK, x[:HALF], x[HALF:])


def lefts_of(matrix):
    lane = lax.broadcasted_iota(jnp.int32, (BLOCK, PAIR), 1)
    high = matrix.astype(jnp.bfloat16).astype(jnp.float32)
    rest = matrix - high
    middle = rest.astype(jnp.bfloat16).astype(jnp.float32)
    first = jnp.where(lane < BLOCK, high, middle)
    second = jnp.where(lane < BLOCK, rest - middle, high)
    return jnp.concatenate([first, second], axis=1).astype(jnp.bfloat16)


def rights_of(block):
    high, low = split(block)
    return jnp.concatenate([high, high, high, low], axis=0)


def opened(packed, block):
    coupling = doubled(packed)
    flipped = jnp.concatenate([coupling, coupling], axis=0).T[:BLOCK]
    rest = block[:BLOCK] - product(lefts_of(coupling), rights_of(block[BLOCK:]))
    return jnp.concatenate(split(rest), axis=0), lefts_of(flipped)


def upper_solved(packed, rest):
    high = rest[:BLOCK]
    return product(lefts_of(doubled(packed)), jnp.concatenate([high, high, rest], axis=0))


def lower_solved(flip, upper, block):
    return block[BLOCK:] + product(flip, rights_of(upper))


def turned(packed, rest, flip, block):
    upper = upper_solved(packed, rest)
    return 2.0 * upper - block[:BLOCK], 2.0 * lower_solved(flip, upper, block) - block[BLOCK:]


def turned_half(packed, rest, flip, block, side):
    upper = upper_solved(packed, rest)
    if side == 0:
        return 2.0 * upper - block[:BLOCK]
    return 2.0 * lower_solved(flip, upper, block) - block[BLOCK:]


def gram_packed(block):
    high, low = split(block)
    lefts = jnp.concatenate([high[:BLOCK], low[:BLOCK]], axis=0)
    rights = jnp.concatenate([high[BLOCK:], low[BLOCK:]], axis=0)
    parts = product(lefts, rights, NT)
    halves = parts[:BLOCK] + parts[BLOCK:]
    cross = halves + pltpu.roll(halves, BLOCK, 1)
    lane = lax.broadcasted_iota(jnp.int32, (HALF, PAIR), 1)
    cross = jnp.where(lane < BLOCK, cross[:HALF], cross[HALF:])
    squares = block * block
    partial = squares[:, :128]
    for start in range(128, squares.shape[1], 128):
        partial = partial + squares[:, start : start + 128]
    norms = jnp.broadcast_to(jnp.sum(partial.T, axis=0, keepdims=True), (8, PAIR))
    rows = lax.broadcasted_iota(jnp.int32, (8, PAIR), 0)
    lanes = lax.broadcasted_iota(jnp.int32, (8, PAIR), 1)
    norms = jnp.where(jnp.logical_and(rows == 1, lanes < BLOCK), pltpu.roll(norms, BLOCK, 1), norms)
    return jnp.concatenate([cross, norms], axis=0)


def kernel(rows, cols, pairs, order_ref, columns_ref, x1, inverses, halo_inverses, rests, flips,
           couplings, halo_couplings, x0, grams, parts, gram_send, gram_recv, coupling_send, coupling_recv, inverse_send,
           inverse_recv, halo_send, halo_recv, start_send, start_recv, edge_send, edge_recv):
    buffers = (x0, x1)
    me = lax.axis_index("row")
    position = lax.axis_index("col")
    partner = jnp.bitwise_xor(me, 1)
    has_left = position > 0
    has_right = position < cols - 1
    has = (has_left, has_right)
    beside = (position - 1, position + 1)
    last = pairs - 1
    kinds = ((couplings, halo_couplings, coupling_send, coupling_recv), (inverses, halo_inverses, inverse_send, inverse_recv))

    barrier = pltpu.get_barrier_semaphore()

    def greet(other, carry):
        @pl.when(other != me)
        def _():
            pl.semaphore_signal(barrier, inc=1, device_id={"row": other})

        for side in (0, 1):
            @pl.when(has[side])
            def _(side=side):
                pl.semaphore_signal(barrier, inc=1, device_id={"row": other, "col": beside[side]})
        return carry

    lax.fori_loop(0, rows, greet, 0)

    def fill(pair):
        for slot in (2 * pair, 2 * pair + 1):
            source = lax.rem(order_ref[slot], 2 * pairs)
            x0[pl.ds(pl.multiple_of(slot * BLOCK + PAIR, BLOCK), BLOCK), :] = columns_ref[source]

    def group_at(place):
        return pairs // 2 - 1 - place, pairs // 2 + place

    fill(0)
    fill(last)
    greeted = rows - 1 + rows * (has_left.astype(jnp.int32) + has_right.astype(jnp.int32))
    pl.semaphore_wait(barrier, greeted)

    def gram_copy(pair):
        return pltpu.make_async_remote_copy(
            src_ref=grams.at[pair, pl.ds(0, HALF + 2)], dst_ref=parts.at[me, pl.ds(0, HALF + 2)], send_sem=gram_send.at[pair], recv_sem=gram_recv.at[me],
            device_id={"row": pair},
        )

    def gram_arrival(source):
        return pltpu.make_async_remote_copy(
            src_ref=parts.at[source, pl.ds(0, HALF + 2)], dst_ref=parts.at[source, pl.ds(0, HALF + 2)], send_sem=gram_send.at[0],
            recv_sem=gram_recv.at[source], device_id={"row": partner},
        )

    def spread_copy(kind, other):
        values, _, send, recv = kinds[kind]
        return pltpu.make_async_remote_copy(
            src_ref=values.at[me], dst_ref=values.at[me], send_sem=send.at[other], recv_sem=recv.at[me],
            device_id={"row": jnp.bitwise_xor(me, other)},
        )

    def spread_arrival(kind, pair):
        values, _, send, recv = kinds[kind]
        return pltpu.make_async_remote_copy(
            src_ref=values.at[pair], dst_ref=values.at[pair], send_sem=send.at[0], recv_sem=recv.at[pair],
            device_id={"row": partner},
        )

    def halo_copy(kind, other, side, now):
        values, halo, _, _ = kinds[kind]
        return pltpu.make_async_remote_copy(
            src_ref=values.at[me], dst_ref=halo.at[now, side], send_sem=halo_send.at[kind, other],
            recv_sem=halo_recv.at[kind, now, side],
            device_id={"row": jnp.bitwise_xor(me, other), "col": beside[1 - side]},
        )

    def halo_arrival(kind, side, now):
        halo = kinds[kind][1]
        return pltpu.make_async_remote_copy(
            src_ref=halo.at[now, side], dst_ref=halo.at[now, side], send_sem=halo_send.at[kind, 0],
            recv_sem=halo_recv.at[kind, now, side], device_id={"row": partner},
        )

    far = (pairs + 1) * PAIR

    def start_copy(side):
        source = pairs * PAIR if side == 0 else PAIR
        target = 0 if side == 0 else far
        return pltpu.make_async_remote_copy(
            src_ref=x0.at[pl.ds(source, PAIR)], dst_ref=x0.at[pl.ds(target, PAIR)], send_sem=start_send.at[side],
            recv_sem=start_recv.at[side], device_id={"col": beside[1 - side]},
        )

    def edge_copy(side, after):
        source = pairs * PAIR if side == 0 else PAIR + BLOCK
        target = 0 if side == 0 else far + BLOCK
        return pltpu.make_async_remote_copy(
            src_ref=buffers[after].at[pl.ds(source, BLOCK)], dst_ref=buffers[after].at[pl.ds(target, BLOCK)],
            send_sem=edge_send.at[after, side], recv_sem=edge_recv.at[after, side],
            device_id={"col": beside[1 - side]},
        )

    for side in (0, 1):
        @pl.when(has[1 - side])
        def _(side=side):
            start_copy(side).start()

    def slot_of(slot, now):
        return buffers[now][pl.ds(pl.multiple_of(slot * PAIR, PAIR), PAIR), :]

    def spread(kind, now):
        def spread_out(place, carry):
            spread_copy(kind, rows - place).start()
            return carry

        lax.fori_loop(1, rows, spread_out, 0)
        for side, owner in ((0, last), (1, 0)):
            @pl.when(jnp.logical_and(me == owner, has[1 - side]))
            def _(side=side):
                def spread_halo(place, carry):
                    halo_copy(kind, rows - place, side, now).start()
                    return carry

                lax.fori_loop(1, rows + 1, spread_halo, 0)

    def settle_spread(kind, now):
        def settle_out(other, carry):
            spread_copy(kind, other).wait_send()
            return carry

        lax.fori_loop(1, rows, settle_out, 0)
        for side, owner in ((0, last), (1, 0)):
            @pl.when(jnp.logical_and(me == owner, has[1 - side]))
            def _(side=side):
                def settle_halo(other, carry):
                    halo_copy(kind, other, side, now).wait_send()
                    return carry

                lax.fori_loop(0, rows, settle_halo, 0)

    def own(now):
        def gather(source, carry):
            @pl.when(source != me)
            def _():
                gram_arrival(source).wait_recv()
            return carry

        lax.fori_loop(0, rows, gather, 0)
        total = grams[me]
        for source in range(rows):
            total = total + jnp.where(source == me, 0.0, parts[source])
        couplings[me] = coupling_packed(total)
        spread(0, now)
        inverses[me] = inverse_packed(couplings[me])
        spread(1, now)

    def take_grams(place, now):
        chosen = group_at(place)
        for pair in chosen:
            grams[pair] = gram_packed(slot_of(pair + 1, now))
        for pair in chosen:
            @pl.when(pair != me)
            def _(pair=pair):
                gram_copy(pair).start()

    def first_grams(place, carry):
        for pair in group_at(place):
            fill(pair)
        take_grams(place, 0)
        return carry

    lax.fori_loop(0, pairs // 2 - 1, first_grams, 0)
    take_grams(pairs // 2 - 1, 0)

    def step(index):
        now, after = index % 2, 1 - index % 2
        later = buffers[after]
        ending = index == STEPS - 1

        @pl.when(me < pairs)
        def _():
            own(now)

        def settle_gram(pair, carry):
            @pl.when(pair != me)
            def _():
                gram_copy(pair).wait_send()
            return carry

        lax.fori_loop(0, pairs, settle_gram, 0)

        for side in (0, 1):
            @pl.when(has[1 - side])
            def _(side=side):
                if index > 1:
                    edge_copy(side, after).wait_send()
                if index == 1:
                    start_copy(side).wait_send()

        def receive(kind, place):
            for pair in group_at(place):
                @pl.when(pair != me)
                def _(pair=pair):
                    spread_arrival(kind, pair).wait_recv()

        def receive_halo(kind, side):
            halo_arrival(kind, side, now).wait_recv()
            if kind == 0:
                if index == 0:
                    start_copy(side).wait_recv()
                else:
                    edge_copy(side, now).wait_recv()

        def open_group(place):
            receive(0, place)
            made = [opened(couplings[pair], slot_of(pair + 1, now)) for pair in group_at(place)]
            for pair, (rest, flip) in zip(group_at(place), made):
                rests[pair + 1], flips[pair + 1] = rest, flip

        def close_group(place):
            receive(1, place)
            chosen = group_at(place)
            results = [turned(inverses[pair], rests[pair + 1], flips[pair + 1], slot_of(pair + 1, now)) for pair in chosen]
            for pair, (upper, lower) in zip(chosen, results):
                opening = jnp.logical_and(pair == 0, jnp.logical_not(has_left))
                closing = jnp.logical_and(pair == last, jnp.logical_not(has_right))
                top = jnp.where(opening, PAIR, jnp.where(closing, pairs * PAIR + BLOCK, (pair + 2) * PAIR))
                bottom = jnp.where(opening, 2 * PAIR, pair * PAIR + BLOCK)
                later[pl.ds(pl.multiple_of(top, BLOCK), BLOCK), :] = upper
                later[pl.ds(pl.multiple_of(bottom, BLOCK), BLOCK), :] = lower

        def receive_halos(kind):
            for side in (0, 1):
                @pl.when(has[side])
                def _(side=side):
                    receive_halo(kind, side)

        def open_halos():
            receive_halos(0)
            made = [opened(halo_couplings[now, side], slot_of(side * (pairs + 1), now)) for side in (0, 1)]
            for side in (0, 1):
                rests[side * (pairs + 1)], flips[side * (pairs + 1)] = made[side]

        def close_halos():
            receive_halos(1)
            slots = (0, pairs + 1)
            made = [
                turned_half(halo_inverses[now, side], rests[slots[side]], flips[slots[side]], slot_of(slots[side], now), side)
                for side in (0, 1)
            ]
            targets = (jnp.where(has_left, PAIR, 0), jnp.where(has_right, pairs * PAIR + BLOCK, far + BLOCK))
            for side in (0, 1):
                later[pl.ds(pl.multiple_of(targets[side], BLOCK), BLOCK), :] = made[side]

        if ending:
            for place in range(pairs // 2):
                open_group(place)
            open_halos()
            for place in range(pairs // 2):
                receive(1, place)
            receive_halos(1)
        else:
            open_group(0)
            open_group(1)
            close_group(0)

            def close_next(place, carry):
                open_group(place + 1)
                close_group(place)
                take_grams(place - 1, after)
                return carry

            lax.fori_loop(1, pairs // 2 - 1, close_next, 0)
            open_halos()
            for side in (0, 1):
                @pl.when(has[1 - side])
                def _(side=side):
                    edge_copy(side, after).start()

            close_group(pairs // 2 - 1)
            take_grams(pairs // 2 - 2, after)
            close_halos()
            take_grams(pairs // 2 - 1, after)
        @pl.when(me < pairs)
        def _():
            for kind in (0, 1):
                settle_spread(kind, now)

    for index in range(STEPS):
        step(index)
    for side in (0, 1):
        @pl.when(has[1 - side])
        def _(side=side):
            edge_copy(side, (STEPS - 1) % 2).wait_send()


def closing_kernel(cols, pairs, x, inverses, halo_inverses, rests, flips, out_ref, result, out_sem):
    position = lax.axis_index("col")
    has = (position > 0, position < cols - 1)
    last = pairs - 1
    now = (STEPS - 1) % 2

    def out_copy(place, row):
        rows = pl.ds(pl.multiple_of(row, BLOCK), BLOCK)
        return pltpu.make_async_copy(result.at[rows], out_ref.at[rows], out_sem.at[place])

    def slot_of(slot):
        return x[pl.ds(pl.multiple_of(slot * PAIR, PAIR), PAIR), :]

    def put(row, values):
        result[pl.ds(pl.multiple_of(row, BLOCK), BLOCK), :] = values

    def finished(pair):
        return turned(inverses[pair], rests[pair + 1], flips[pair + 1], slot_of(pair + 1))

    def finished_half(side):
        slot = side * (pairs + 1)
        return turned_half(halo_inverses[now, side], rests[slot], flips[slot], slot_of(slot), side)

    spare = (pairs * PAIR, pairs * PAIR + BLOCK)
    given = (0, last * PAIR + BLOCK)
    halfway = pairs // 2

    def inner(chosen):
        results = [finished(pair) for pair in chosen]
        for pair, (upper, lower) in zip(chosen, results):
            put((pair + 1) * PAIR, upper)
            put((pair - 1) * PAIR + BLOCK, lower)

    def send_inner(chosen):
        for pair in chosen:
            out_copy(2 * pair, (pair + 1) * PAIR).start()
            out_copy(2 * pair + 1, (pair - 1) * PAIR + BLOCK).start()

    sets = (tuple(range(1, halfway + 1)), tuple(range(halfway + 1, last)))
    inner(sets[0])
    send_inner(sets[0])
    inner(sets[1])
    first_top = jnp.where(has[0], PAIR, 0)
    lowest = (last - 1) * PAIR + BLOCK
    kept = (jnp.where(has[0], spare[0], PAIR), jnp.where(has[1], spare[1], last * PAIR + BLOCK))
    results = [finished(pair) for pair in (0, last)]
    halves = [finished_half(side) for side in (0, 1)]
    put(first_top, results[0][0])
    put(lowest, results[1][1])
    put(kept[0], results[0][1])
    put(kept[1], results[1][0])
    for side in (0, 1):
        put(jnp.where(has[side], given[side], spare[side]), halves[side])
    send_inner(sets[1])
    out_copy(0, first_top).start()
    out_copy(1, lowest).start()
    for side in (0, 1):
        out_copy(2 * last + side, jnp.where(has[side], given[side], kept[side])).start()

    def settle(place, carry):
        out_copy(place, 0).wait()
        return carry

    lax.fori_loop(0, 2 * pairs, settle, 0)


def solution(mesh):
    rows, cols = mesh.shape["row"], mesh.shape["col"]

    def local(columns, block_order):
        width, length = columns.shape
        pairs = width // PAIR
        assert 4 <= pairs <= rows and rows % pairs == 0 and rows & (rows - 1) == 0 and STEPS % 2 == 0
        dma = pltpu.SemaphoreType.DMA
        wide = (width + 2 * PAIR, length)
        vmem = pl.BlockSpec(memory_space=pltpu.VMEM)
        state = pl.pallas_call(
            functools.partial(kernel, rows, cols, pairs),
            out_shape=[
                jax.ShapeDtypeStruct(wide, jnp.float32),
                jax.ShapeDtypeStruct((pairs, HALF, PAIR), jnp.float32),
                jax.ShapeDtypeStruct((2, 2, HALF, PAIR), jnp.float32),
                jax.ShapeDtypeStruct((pairs + 2, 2 * BLOCK, length), jnp.bfloat16),
                jax.ShapeDtypeStruct((pairs + 2, BLOCK, 2 * PAIR), jnp.bfloat16),
            ],
            in_specs=[pl.BlockSpec(memory_space=pltpu.SMEM), vmem],
            out_specs=[vmem] * 5,
            scratch_shapes=[
                pltpu.VMEM((pairs, HALF, PAIR), jnp.float32),
                pltpu.VMEM((2, 2, HALF, PAIR), jnp.float32),
                pltpu.VMEM(wide, jnp.float32),
                pltpu.VMEM((pairs, PACKED, PAIR), jnp.float32),
                pltpu.VMEM((rows, PACKED, PAIR), jnp.float32),
                dma((pairs,)),
                dma((rows,)),
                dma((rows,)),
                dma((pairs,)),
                dma((rows,)),
                dma((pairs,)),
                dma((2, rows)),
                dma((2, 2, 2)),
                dma((2,)),
                dma((2,)),
                dma((2, 2)),
                dma((2, 2)),
            ],
            compiler_params=pltpu.CompilerParams(
                collective_id=0, has_side_effects=True, vmem_limit_bytes=20 * 1024 * 1024
            ),
        )(block_order, columns.reshape(2 * pairs, BLOCK, length))
        return pl.pallas_call(
            functools.partial(closing_kernel, cols, pairs),
            out_shape=jax.ShapeDtypeStruct((width, length), jnp.float32),
            in_specs=[vmem] * 5,
            out_specs=pl.BlockSpec(memory_space=pl.ANY),
            scratch_shapes=[pltpu.VMEM((width + PAIR, length), jnp.float32), dma((2 * pairs,))],
            compiler_params=pltpu.CompilerParams(vmem_limit_bytes=20 * 1024 * 1024),
        )(*state)

    placed = (P("col", "row"), P("col"))
    return jax.shard_map(local, mesh=mesh, in_specs=placed, out_specs=P("col", "row"), check_vma=False)
```

```python
import functools

import jax
import jax.numpy as jnp
from jax import lax
from jax.experimental import pallas as pl
from jax.experimental.pallas import tpu as pltpu
from jax.sharding import PartitionSpec as P

BLOCK = 64
PAIR = 2 * BLOCK
STEPS = 4
HALF = BLOCK // 2
PACKED = HALF + 8
UPPER = 1.0 + BLOCK * BLOCK * 0.0905
NN = (((1,), (0,)), ((), ()))
NT = (((1,), (1,)), ((), ()))


def split(a):
    high = a.astype(jnp.bfloat16)
    return high, (a - high.astype(jnp.float32)).astype(jnp.bfloat16)


def split3(a):
    high = a.astype(jnp.bfloat16)
    rest = a - high.astype(jnp.float32)
    middle = rest.astype(jnp.bfloat16)
    return high, middle, (rest - middle.astype(jnp.float32)).astype(jnp.bfloat16)


def product(a, b, dims=NN):
    return lax.dot_general(a, b, dims, preferred_element_type=jnp.float32)


def mm3(a, b, dims=NN):
    (ah, am), (bh, bm) = split(a), split(b)
    count = a.shape[0]
    stacked = product(jnp.concatenate([ah, am], axis=0), bh, dims)
    return stacked[:count] + stacked[count:] + product(ah, bm, dims)


def mm6(a, b, dims=NN):
    (ah, am, al), (bh, bm, bl) = split3(a), split3(b)
    count = a.shape[0]
    first = product(jnp.concatenate([ah, am, al], axis=0), bh, dims)
    second = product(jnp.concatenate([ah, am], axis=0), bm, dims)
    small = first[2 * count :] + second[count:] + product(ah, bl, dims)
    return first[:count] + ((first[count : 2 * count] + second[:count]) + small)


def left(a):
    return a[:, :BLOCK]


def inverse(system, eye):
    low = 2.0 / (1.0 + UPPER)
    y = system * low
    reach = low * (2.0 - low)
    scale = 2.0 / (1.0 + reach)
    x = (scale * low) * (2.0 * eye - y)
    y = scale * (2.0 * y - mm3(left(y), y))
    low = scale * reach
    while low < 0.999:
        reach = low * (2.0 - low)
        scale = 2.0 / (1.0 + reach)
        following = scale * (2.0 * y - mm3(left(y), y))
        x = scale * (2.0 * x - mm3(left(x), y))
        y = following
        low = scale * reach
    return x


def coupling_packed(total):
    row = lax.broadcasted_iota(jnp.int32, (HALF, PAIR), 0)
    lane = lax.broadcasted_iota(jnp.int32, (HALF, PAIR), 1)
    cross = total[:HALF]
    norms = total[HALF : HALF + 1]
    bottom_norms = total[HALF + 1 : HALF + 2]
    upper_norms = jnp.sum(jnp.where(lane == row, norms, 0.0), axis=1, keepdims=True)
    lower_norms = jnp.sum(jnp.where(lane == row + HALF, norms, 0.0), axis=1, keepdims=True)
    top_norms = jnp.where(lane < BLOCK, upper_norms, lower_norms)
    spread = bottom_norms - top_norms
    square = spread * spread + 4.0 * cross * cross
    radius = jnp.sqrt(square)
    scale_term = (top_norms + bottom_norms) / BLOCK
    return 2.0 * cross * spread / (square + jnp.abs(spread) * radius + scale_term * scale_term)


def doubled(packed):
    lane = lax.broadcasted_iota(jnp.int32, (HALF, PAIR), 1)
    rolled = pltpu.roll(packed, BLOCK, 1)
    return jnp.concatenate([jnp.where(lane < BLOCK, packed, rolled), jnp.where(lane < BLOCK, rolled, packed)], axis=0)


def inverse_packed(packed):
    coupling = doubled(packed)
    rows = lax.broadcasted_iota(jnp.int32, (BLOCK, PAIR), 0)
    lanes = lax.broadcasted_iota(jnp.int32, (BLOCK, PAIR), 1)
    columns = jnp.where(lanes < BLOCK, lanes, lanes - BLOCK)
    eye = jnp.where(rows == columns, 1.0, 0.0).astype(jnp.float32)
    narrow = left(coupling)
    narrow_t = narrow.T
    system = eye + mm3(narrow, jnp.concatenate([narrow, narrow], axis=0), NT)
    x = inverse(system, eye)
    residual = eye - x - mm6(narrow, mm6(narrow_t, x))
    x = x + mm3(left(x), residual)
    return jnp.where(lanes[:HALF] < BLOCK, x[:HALF], x[HALF:])


def lefts_of(matrix):
    lane = lax.broadcasted_iota(jnp.int32, (BLOCK, PAIR), 1)
    high = matrix.astype(jnp.bfloat16).astype(jnp.float32)
    rest = matrix - high
    middle = rest.astype(jnp.bfloat16).astype(jnp.float32)
    first = jnp.where(lane < BLOCK, high, middle)
    second = jnp.where(lane < BLOCK, rest - middle, high)
    return jnp.concatenate([first, second], axis=1).astype(jnp.bfloat16)


def rights_of(block):
    high, low = split(block)
    return jnp.concatenate([high, high, high, low], axis=0)


def opened(packed, block):
    coupling = doubled(packed)
    flipped = jnp.concatenate([coupling, coupling], axis=0).T[:BLOCK]
    rest = block[:BLOCK] - product(lefts_of(coupling), rights_of(block[BLOCK:]))
    return jnp.concatenate(split(rest), axis=0), lefts_of(flipped)


def upper_solved(packed, rest):
    high = rest[:BLOCK]
    return product(lefts_of(doubled(packed)), jnp.concatenate([high, high, rest], axis=0))


def lower_solved(flip, upper, block):
    return block[BLOCK:] + product(flip, rights_of(upper))


def turned(packed, rest, flip, block):
    upper = upper_solved(packed, rest)
    return 2.0 * upper - block[:BLOCK], 2.0 * lower_solved(flip, upper, block) - block[BLOCK:]


def turned_half(packed, rest, flip, block, side):
    upper = upper_solved(packed, rest)
    if side == 0:
        return 2.0 * upper - block[:BLOCK]
    return 2.0 * lower_solved(flip, upper, block) - block[BLOCK:]


def gram_packed(block):
    high, low = split(block)
    lefts = jnp.concatenate([high[:BLOCK], low[:BLOCK]], axis=0)
    rights = jnp.concatenate([high[BLOCK:], low[BLOCK:]], axis=0)
    parts = product(lefts, rights, NT)
    halves = parts[:BLOCK] + parts[BLOCK:]
    cross = halves + pltpu.roll(halves, BLOCK, 1)
    lane = lax.broadcasted_iota(jnp.int32, (HALF, PAIR), 1)
    cross = jnp.where(lane < BLOCK, cross[:HALF], cross[HALF:])
    squares = block * block
    partial = squares[:, :128]
    for start in range(128, squares.shape[1], 128):
        partial = partial + squares[:, start : start + 128]
    norms = jnp.broadcast_to(jnp.sum(partial.T, axis=0, keepdims=True), (8, PAIR))
    rows = lax.broadcasted_iota(jnp.int32, (8, PAIR), 0)
    lanes = lax.broadcasted_iota(jnp.int32, (8, PAIR), 1)
    norms = jnp.where(jnp.logical_and(rows == 1, lanes < BLOCK), pltpu.roll(norms, BLOCK, 1), norms)
    return jnp.concatenate([cross, norms], axis=0)


def kernel(rows, cols, pairs, order_ref, columns_ref, x1, inverses, halo_inverses, rests, flips,
           couplings, halo_couplings, x0, grams, parts, gram_send, gram_recv, coupling_send, coupling_recv, inverse_send,
           inverse_recv, halo_send, halo_recv, start_send, start_recv, edge_send, edge_recv):
    buffers = (x0, x1)
    me = lax.axis_index("row")
    position = lax.axis_index("col")
    partner = jnp.bitwise_xor(me, 1)
    has_left = position > 0
    has_right = position < cols - 1
    has = (has_left, has_right)
    beside = (position - 1, position + 1)
    last = pairs - 1
    kinds = ((couplings, halo_couplings, coupling_send, coupling_recv), (inverses, halo_inverses, inverse_send, inverse_recv))

    barrier = pltpu.get_barrier_semaphore()

    def greet(other, carry):
        @pl.when(other != me)
        def _():
            pl.semaphore_signal(barrier, inc=1, device_id={"row": other})

        for side in (0, 1):
            @pl.when(has[side])
            def _(side=side):
                pl.semaphore_signal(barrier, inc=1, device_id={"row": other, "col": beside[side]})
        return carry

    lax.fori_loop(0, rows, greet, 0)

    def fill(pair):
        for slot in (2 * pair, 2 * pair + 1):
            source = lax.rem(order_ref[slot], 2 * pairs)
            x0[pl.ds(pl.multiple_of(slot * BLOCK + PAIR, BLOCK), BLOCK), :] = columns_ref[source]

    def group_at(place):
        return pairs // 2 - 1 - place, pairs // 2 + place

    fill(0)
    fill(last)
    greeted = rows - 1 + rows * (has_left.astype(jnp.int32) + has_right.astype(jnp.int32))
    pl.semaphore_wait(barrier, greeted)

    def gram_copy(pair):
        return pltpu.make_async_remote_copy(
            src_ref=grams.at[pair, pl.ds(0, HALF + 2)], dst_ref=parts.at[me, pl.ds(0, HALF + 2)], send_sem=gram_send.at[pair], recv_sem=gram_recv.at[me],
            device_id={"row": pair},
        )

    def gram_arrival(source):
        return pltpu.make_async_remote_copy(
            src_ref=parts.at[source, pl.ds(0, HALF + 2)], dst_ref=parts.at[source, pl.ds(0, HALF + 2)], send_sem=gram_send.at[0],
            recv_sem=gram_recv.at[source], device_id={"row": partner},
        )

    def spread_copy(kind, other):
        values, _, send, recv = kinds[kind]
        return pltpu.make_async_remote_copy(
            src_ref=values.at[me], dst_ref=values.at[me], send_sem=send.at[other], recv_sem=recv.at[me],
            device_id={"row": jnp.bitwise_xor(me, other)},
        )

    def spread_arrival(kind, pair):
        values, _, send, recv = kinds[kind]
        return pltpu.make_async_remote_copy(
            src_ref=values.at[pair], dst_ref=values.at[pair], send_sem=send.at[0], recv_sem=recv.at[pair],
            device_id={"row": partner},
        )

    def halo_copy(kind, other, side, now):
        values, halo, _, _ = kinds[kind]
        return pltpu.make_async_remote_copy(
            src_ref=values.at[me], dst_ref=halo.at[now, side], send_sem=halo_send.at[kind, other],
            recv_sem=halo_recv.at[kind, now, side],
            device_id={"row": jnp.bitwise_xor(me, other), "col": beside[1 - side]},
        )

    def halo_arrival(kind, side, now):
        halo = kinds[kind][1]
        return pltpu.make_async_remote_copy(
            src_ref=halo.at[now, side], dst_ref=halo.at[now, side], send_sem=halo_send.at[kind, 0],
            recv_sem=halo_recv.at[kind, now, side], device_id={"row": partner},
        )

    far = (pairs + 1) * PAIR

    parts_of = ((0, PAIR - HALF), (PAIR - HALF, HALF))

    def start_copy(side, part):
        first, count = parts_of[part]
        source = pairs * PAIR if side == 0 else PAIR
        target = 0 if side == 0 else far
        return pltpu.make_async_remote_copy(
            src_ref=x0.at[pl.ds(source + first, count)], dst_ref=x0.at[pl.ds(target + first, count)],
            send_sem=start_send.at[part, side], recv_sem=start_recv.at[part, side],
            device_id={"col": beside[1 - side]},
        )

    def edge_copy(side, after):
        source = pairs * PAIR if side == 0 else PAIR + BLOCK
        target = 0 if side == 0 else far + BLOCK
        return pltpu.make_async_remote_copy(
            src_ref=buffers[after].at[pl.ds(source, BLOCK)], dst_ref=buffers[after].at[pl.ds(target, BLOCK)],
            send_sem=edge_send.at[after, side], recv_sem=edge_recv.at[after, side],
            device_id={"col": beside[1 - side]},
        )

    for side in (0, 1):
        @pl.when(has[1 - side])
        def _(side=side):
            start_copy(side, 0).start()

    def slot_of(slot, now):
        return buffers[now][pl.ds(pl.multiple_of(slot * PAIR, PAIR), PAIR), :]

    def spread(kind, now):
        def spread_out(place, carry):
            spread_copy(kind, rows - place).start()
            return carry

        lax.fori_loop(1, rows, spread_out, 0)
        for side, owner in ((0, last), (1, 0)):
            @pl.when(jnp.logical_and(me == owner, has[1 - side]))
            def _(side=side):
                def spread_halo(place, carry):
                    halo_copy(kind, rows - place, side, now).start()
                    return carry

                lax.fori_loop(1, rows + 1, spread_halo, 0)

    def settle_spread(kind, now):
        def settle_out(other, carry):
            spread_copy(kind, other).wait_send()
            return carry

        lax.fori_loop(1, rows, settle_out, 0)
        for side, owner in ((0, last), (1, 0)):
            @pl.when(jnp.logical_and(me == owner, has[1 - side]))
            def _(side=side):
                def settle_halo(other, carry):
                    halo_copy(kind, other, side, now).wait_send()
                    return carry

                lax.fori_loop(0, rows, settle_halo, 0)

    def own(now):
        def gather(source, carry):
            @pl.when(source != me)
            def _():
                gram_arrival(source).wait_recv()
            return carry

        lax.fori_loop(0, rows, gather, 0)
        total = grams[me]
        for source in range(rows):
            total = total + jnp.where(source == me, 0.0, parts[source])
        couplings[me] = coupling_packed(total)
        spread(0, now)
        inverses[me] = inverse_packed(couplings[me])
        spread(1, now)

    def take_grams(place, now):
        chosen = group_at(place)
        for pair in chosen:
            grams[pair] = gram_packed(slot_of(pair + 1, now))
        for pair in chosen:
            @pl.when(pair != me)
            def _(pair=pair):
                gram_copy(pair).start()

    def first_grams(place, carry):
        for pair in group_at(place):
            fill(pair)
        take_grams(place, 0)
        return carry

    lax.fori_loop(0, pairs // 2 - 1, first_grams, 0)
    take_grams(pairs // 2 - 1, 0)

    def step(index):
        now, after = index % 2, 1 - index % 2
        later = buffers[after]
        ending = index == STEPS - 1

        @pl.when(me < pairs)
        def _():
            own(now)

        if index == 0:
            for side in (0, 1):
                @pl.when(has[1 - side])
                def _(side=side):
                    start_copy(side, 1).start()

        def settle_gram(pair, carry):
            @pl.when(pair != me)
            def _():
                gram_copy(pair).wait_send()
            return carry

        lax.fori_loop(0, pairs, settle_gram, 0)

        for side in (0, 1):
            @pl.when(has[1 - side])
            def _(side=side):
                if index > 1:
                    edge_copy(side, after).wait_send()
                if index == 1:
                    start_copy(side, 0).wait_send()
                    start_copy(side, 1).wait_send()

        def receive(kind, place):
            for pair in group_at(place):
                @pl.when(pair != me)
                def _(pair=pair):
                    spread_arrival(kind, pair).wait_recv()

        def receive_halo(kind, side):
            halo_arrival(kind, side, now).wait_recv()
            if kind == 0:
                if index == 0:
                    start_copy(side, 0).wait_recv()
                    start_copy(side, 1).wait_recv()
                else:
                    edge_copy(side, now).wait_recv()

        def open_group(place):
            receive(0, place)
            made = [opened(couplings[pair], slot_of(pair + 1, now)) for pair in group_at(place)]
            for pair, (rest, flip) in zip(group_at(place), made):
                rests[pair + 1], flips[pair + 1] = rest, flip

        def close_group(place):
            receive(1, place)
            chosen = group_at(place)
            results = [turned(inverses[pair], rests[pair + 1], flips[pair + 1], slot_of(pair + 1, now)) for pair in chosen]
            for pair, (upper, lower) in zip(chosen, results):
                opening = jnp.logical_and(pair == 0, jnp.logical_not(has_left))
                closing = jnp.logical_and(pair == last, jnp.logical_not(has_right))
                top = jnp.where(opening, PAIR, jnp.where(closing, pairs * PAIR + BLOCK, (pair + 2) * PAIR))
                bottom = jnp.where(opening, 2 * PAIR, pair * PAIR + BLOCK)
                later[pl.ds(pl.multiple_of(top, BLOCK), BLOCK), :] = upper
                later[pl.ds(pl.multiple_of(bottom, BLOCK), BLOCK), :] = lower

        def receive_halos(kind):
            for side in (0, 1):
                @pl.when(has[side])
                def _(side=side):
                    receive_halo(kind, side)

        def open_halos():
            receive_halos(0)
            made = [opened(halo_couplings[now, side], slot_of(side * (pairs + 1), now)) for side in (0, 1)]
            for side in (0, 1):
                rests[side * (pairs + 1)], flips[side * (pairs + 1)] = made[side]

        def close_halos():
            receive_halos(1)
            slots = (0, pairs + 1)
            made = [
                turned_half(halo_inverses[now, side], rests[slots[side]], flips[slots[side]], slot_of(slots[side], now), side)
                for side in (0, 1)
            ]
            targets = (jnp.where(has_left, PAIR, 0), jnp.where(has_right, pairs * PAIR + BLOCK, far + BLOCK))
            for side in (0, 1):
                later[pl.ds(pl.multiple_of(targets[side], BLOCK), BLOCK), :] = made[side]

        if ending:
            for place in range(pairs // 2):
                open_group(place)
            open_halos()
            for place in range(pairs // 2):
                receive(1, place)
            receive_halos(1)
        else:
            open_group(0)
            open_group(1)
            close_group(0)

            def close_next(place, carry):
                open_group(place + 1)
                close_group(place)
                take_grams(place - 1, after)
                return carry

            lax.fori_loop(1, pairs // 2 - 1, close_next, 0)
            open_halos()
            for side in (0, 1):
                @pl.when(has[1 - side])
                def _(side=side):
                    edge_copy(side, after).start()

            close_group(pairs // 2 - 1)
            take_grams(pairs // 2 - 2, after)
            close_halos()
            take_grams(pairs // 2 - 1, after)
        @pl.when(me < pairs)
        def _():
            for kind in (0, 1):
                settle_spread(kind, now)

    for index in range(STEPS):
        step(index)
    for side in (0, 1):
        @pl.when(has[1 - side])
        def _(side=side):
            edge_copy(side, (STEPS - 1) % 2).wait_send()


def closing_kernel(cols, pairs, x, inverses, halo_inverses, rests, flips, out_ref, result, out_sem):
    position = lax.axis_index("col")
    has = (position > 0, position < cols - 1)
    last = pairs - 1
    now = (STEPS - 1) % 2

    def out_copy(place, row):
        rows = pl.ds(pl.multiple_of(row, BLOCK), BLOCK)
        return pltpu.make_async_copy(result.at[rows], out_ref.at[rows], out_sem.at[place])

    def slot_of(slot):
        return x[pl.ds(pl.multiple_of(slot * PAIR, PAIR), PAIR), :]

    def put(row, values):
        result[pl.ds(pl.multiple_of(row, BLOCK), BLOCK), :] = values

    def finished(pair):
        return turned(inverses[pair], rests[pair + 1], flips[pair + 1], slot_of(pair + 1))

    def finished_half(side):
        slot = side * (pairs + 1)
        return turned_half(halo_inverses[now, side], rests[slot], flips[slot], slot_of(slot), side)

    spare = (pairs * PAIR, pairs * PAIR + BLOCK)
    given = (0, last * PAIR + BLOCK)
    halfway = pairs // 2

    def inner(chosen):
        results = [finished(pair) for pair in chosen]
        for pair, (upper, lower) in zip(chosen, results):
            put((pair + 1) * PAIR, upper)
            put((pair - 1) * PAIR + BLOCK, lower)

    def send_inner(chosen):
        for pair in chosen:
            out_copy(2 * pair, (pair + 1) * PAIR).start()
            out_copy(2 * pair + 1, (pair - 1) * PAIR + BLOCK).start()

    sets = (tuple(range(1, halfway + 1)), tuple(range(halfway + 1, last)))
    inner(sets[0])
    send_inner(sets[0])
    inner(sets[1])
    first_top = jnp.where(has[0], PAIR, 0)
    lowest = (last - 1) * PAIR + BLOCK
    kept = (jnp.where(has[0], spare[0], PAIR), jnp.where(has[1], spare[1], last * PAIR + BLOCK))
    results = [finished(pair) for pair in (0, last)]
    halves = [finished_half(side) for side in (0, 1)]
    put(first_top, results[0][0])
    put(lowest, results[1][1])
    put(kept[0], results[0][1])
    put(kept[1], results[1][0])
    for side in (0, 1):
        put(jnp.where(has[side], given[side], spare[side]), halves[side])
    send_inner(sets[1])
    out_copy(0, first_top).start()
    out_copy(1, lowest).start()
    for side in (0, 1):
        out_copy(2 * last + side, jnp.where(has[side], given[side], kept[side])).start()

    def settle(place, carry):
        out_copy(place, 0).wait()
        return carry

    lax.fori_loop(0, 2 * pairs, settle, 0)


def solution(mesh):
    rows, cols = mesh.shape["row"], mesh.shape["col"]

    def local(columns, block_order):
        width, length = columns.shape
        pairs = width // PAIR
        assert 4 <= pairs <= rows and rows % pairs == 0 and rows & (rows - 1) == 0 and STEPS % 2 == 0
        dma = pltpu.SemaphoreType.DMA
        wide = (width + 2 * PAIR, length)
        vmem = pl.BlockSpec(memory_space=pltpu.VMEM)
        state = pl.pallas_call(
            functools.partial(kernel, rows, cols, pairs),
            out_shape=[
                jax.ShapeDtypeStruct(wide, jnp.float32),
                jax.ShapeDtypeStruct((pairs, HALF, PAIR), jnp.float32),
                jax.ShapeDtypeStruct((2, 2, HALF, PAIR), jnp.float32),
                jax.ShapeDtypeStruct((pairs + 2, 2 * BLOCK, length), jnp.bfloat16),
                jax.ShapeDtypeStruct((pairs + 2, BLOCK, 2 * PAIR), jnp.bfloat16),
            ],
            in_specs=[pl.BlockSpec(memory_space=pltpu.SMEM), vmem],
            out_specs=[vmem] * 5,
            scratch_shapes=[
                pltpu.VMEM((pairs, HALF, PAIR), jnp.float32),
                pltpu.VMEM((2, 2, HALF, PAIR), jnp.float32),
                pltpu.VMEM(wide, jnp.float32),
                pltpu.VMEM((pairs, PACKED, PAIR), jnp.float32),
                pltpu.VMEM((rows, PACKED, PAIR), jnp.float32),
                dma((pairs,)),
                dma((rows,)),
                dma((rows,)),
                dma((pairs,)),
                dma((rows,)),
                dma((pairs,)),
                dma((2, rows)),
                dma((2, 2, 2)),
                dma((2, 2)),
                dma((2, 2)),
                dma((2, 2)),
                dma((2, 2)),
            ],
            compiler_params=pltpu.CompilerParams(
                collective_id=0, has_side_effects=True, vmem_limit_bytes=20 * 1024 * 1024
            ),
        )(block_order, columns.reshape(2 * pairs, BLOCK, length))
        return pl.pallas_call(
            functools.partial(closing_kernel, cols, pairs),
            out_shape=jax.ShapeDtypeStruct((width, length), jnp.float32),
            in_specs=[vmem] * 5,
            out_specs=pl.BlockSpec(memory_space=pl.ANY),
            scratch_shapes=[pltpu.VMEM((width + PAIR, length), jnp.float32), dma((2 * pairs,))],
            compiler_params=pltpu.CompilerParams(vmem_limit_bytes=20 * 1024 * 1024),
        )(*state)

    placed = (P("col", "row"), P("col"))
    return jax.shard_map(local, mesh=mesh, in_specs=placed, out_specs=P("col", "row"), check_vma=False)
```
